128 devices in a mesh: dp: 1, tp: 64 (over z, y, x), cp: 2 (over core).
Axes of the slice: x: 4, y: 4, z: 4, core: 2. Of those that a mesh axis runs over, the one named last changes fastest.
Arguments:
- c_latent: bfloat16 [4096, 512], P(('dp', 'cp'))
- k_rope: bfloat16 [4096, 64], P(('dp', 'cp'))
- q_heads: bfloat16 [4096, 128, 192], P(('dp', 'cp'), 'tp')
- d_out: bfloat16 [4096, 128, 128], P(('dp', 'cp'), 'tp')
- w_uk: bfloat16 [512, 128, 128], P(None, 'tp')
- w_uv: bfloat16 [512, 128, 128], P(None, 'tp')
Outputs:
- output 1: bfloat16 [4096, 128, 128], P(('dp', 'cp'), 'tp')
- output 2: float32 [4096, 128, 192], P(('dp', 'cp'), 'tp')
- output 3: float32 [4096, 512], P(('dp', 'cp'))
- output 4: float32 [4096, 64], P(('dp', 'cp'))
- output 5: float32 [512, 128, 128], P('dp', 'tp')
- output 6: float32 [512, 128, 128], P('dp', 'tp')
All inputs are finite; a program needn't handle non-finite values.
Results may differ from the reference program's by a relative error of at most 0.0114719.
Values are sent between devices in bfloat16 or wider.
A program may use at most 1 GiB of HBM per device.

```python
import jax
import jax.numpy as jnp
from jax import lax

TOK_DEV = 2048
CP_SIZE = 2
HEADS = 128
KV_RANK = 512
ROPE_DIM = 64
NOPE_DIM = 128
V_DIM = 128

SEQ_LEN = CP_SIZE * TOK_DEV
HALF_LEN = TOK_DEV // 2
N_PIECES = 2 * CP_SIZE
QK_DIM = NOPE_DIM + ROPE_DIM
NEG_BIG = -1.0e30


def setup_inputs(seed: int = 0, part: int = 0) -> dict:
    base_key = jax.random.key(seed)
    part_key = jax.random.fold_in(base_key, part)
    key_c, key_rope, key_q, key_dout = jax.random.split(part_key, 4)
    key_wk, key_wv = jax.random.split(jax.random.key(seed + 7919), 2)
    c_latent = jax.random.normal(key_c, (SEQ_LEN, KV_RANK), jnp.float32)
    k_rope = jax.random.normal(key_rope, (SEQ_LEN, ROPE_DIM), jnp.float32)
    q_heads = 2.0 * jax.random.normal(key_q, (SEQ_LEN, HEADS, QK_DIM), jnp.float32)
    d_out = jax.random.normal(key_dout, (SEQ_LEN, HEADS, V_DIM), jnp.float32)
    w_uk = jax.random.normal(key_wk, (KV_RANK, HEADS, NOPE_DIM), jnp.float32) * KV_RANK ** -0.5
    w_uv = jax.random.normal(key_wv, (KV_RANK, HEADS, V_DIM), jnp.float32) * KV_RANK ** -0.5
    return {
        'c_latent': c_latent.astype(jnp.bfloat16),
        'k_rope': k_rope.astype(jnp.bfloat16),
        'q_heads': q_heads.astype(jnp.bfloat16),
        'd_out': d_out.astype(jnp.bfloat16),
        'w_uk': w_uk.astype(jnp.bfloat16),
        'w_uv': w_uv.astype(jnp.bfloat16),
    }


def row_positions():
    row_ids = jnp.arange(SEQ_LEN)
    shard_idx = row_ids // TOK_DEV
    within = row_ids % TOK_DEV
    piece_idx = jnp.where(within < HALF_LEN, shard_idx, N_PIECES - 1 - shard_idx)
    return piece_idx * HALF_LEN + within % HALF_LEN


def attend(q_all, knope_all, rope_all, v_all):
    positions = row_positions()
    pos_pieces = positions.reshape(N_PIECES, HALF_LEN)
    qk_scale = QK_DIM ** -0.5

    def head_fn(head_args):
        q_head, knope_head, v_head = head_args
        key_rows = jnp.concatenate([knope_head, rope_all], axis=-1)

        def piece_fn(piece_args):
            q_blk, pos_blk = piece_args
            scores = jnp.dot(q_blk, key_rows.T, preferred_element_type=jnp.float32) * qk_scale
            scores = jnp.where(positions[None, :] <= pos_blk[:, None], scores, NEG_BIG)
            weights = jax.nn.softmax(scores, axis=-1)
            return jnp.dot(weights, v_head, preferred_element_type=jnp.float32)

        out_pieces = lax.map(jax.checkpoint(piece_fn), (q_head.reshape(N_PIECES, HALF_LEN, QK_DIM), pos_pieces))
        return out_pieces.reshape(SEQ_LEN, V_DIM)

    heads_out = lax.map(jax.checkpoint(head_fn), (jnp.transpose(q_all, (1, 0, 2)), jnp.transpose(knope_all, (1, 0, 2)), jnp.transpose(v_all, (1, 0, 2))))
    return jnp.transpose(heads_out, (1, 0, 2))


def reference(c_latent, k_rope, q_heads, d_out, w_uk, w_uv):
    c_wide = c_latent.astype(jnp.float32)
    wk_wide = w_uk.astype(jnp.float32)
    wv_wide = w_uv.astype(jnp.float32)
    knope_all = jnp.einsum('sr,rhd->shd', c_wide, wk_wide).astype(jnp.bfloat16).astype(jnp.float32)
    v_all = jnp.einsum('sr,rhd->shd', c_wide, wv_wide).astype(jnp.bfloat16).astype(jnp.float32)
    out_wide, vjp_fn = jax.vjp(attend, q_heads.astype(jnp.float32), knope_all, k_rope.astype(jnp.float32), v_all)
    dq_heads, dk_nope, dk_rope, dv_all = vjp_fn(d_out.astype(jnp.float32))
    dc_latent = jnp.einsum('shd,rhd->sr', dk_nope, wk_wide) + jnp.einsum('shd,rhd->sr', dv_all, wv_wide)
    dw_uk = jnp.einsum('sr,shd->rhd', c_wide, dk_nope)
    dw_uv = jnp.einsum('sr,shd->rhd', c_wide, dv_all)
    return (out_wide.astype(jnp.bfloat16), dq_heads, dc_latent, dk_rope, dw_uk, dw_uv)
```

```python
import functools
import math

import jax
import jax.numpy as jnp
from jax import lax
from jax.experimental import pallas as pl
from jax.experimental.pallas import tpu as pltpu
from jax.sharding import PartitionSpec as P

BF = jnp.bfloat16
F32 = jnp.float32
NEG_BIG = -1.0e30
LOG2E = math.log2(math.e)


def mm(a, b):
    return lax.dot_general(a, b, (((1,), (0,)), ((), ())), preferred_element_type=F32)


def mm_nt(a, b):
    return lax.dot_general(a, b, (((1,), (1,)), ((), ())), preferred_element_type=F32)


def mm_tn(a, b):
    return lax.dot_general(a, b, (((0,), (0,)), ((), ())), preferred_element_type=F32)


def fwd_kernel(blk, dn, dv, c_ref, r_ref, q_ref, do_ref, wuk_ref, wuv_ref,
               o_ref, lse_ref, dd_ref, kc_ref, v_ref, kt_ref, vt_scr, kc_scr, m_scr, l_scr, acc_scr):
    i = pl.program_id(0)
    qk = q_ref.shape[1]
    scale2 = (qk ** -0.5) * LOG2E
    kb = mm(c_ref[...], wuk_ref[...]).astype(BF)
    vb = mm(c_ref[...], wuv_ref[...])
    rows = pl.ds(pl.multiple_of(i * blk, blk), blk)
    kc_scr[rows, :dn] = kb
    kc_scr[rows, dn:] = r_ref[...]
    kc_ref[:, :dn] = kb
    kc_ref[:, dn:] = r_ref[...]
    v_ref[...] = vb.astype(BF)
    vt_scr[i] = vb.T.astype(BF)
    kcv = kc_scr[rows, :]
    kt_ref[...] = kcv.astype(F32).T.astype(BF)[None]

    def update(j, masked, first):
        ks = pl.ds(pl.multiple_of(j * blk, blk), blk)
        s = mm_nt(kc_scr[ks, :], q_ref[...])
        if masked:
            kpos = lax.broadcasted_iota(jnp.int32, (blk, blk), 0)
            qpos = lax.broadcasted_iota(jnp.int32, (blk, blk), 1)
            s = jnp.where(kpos <= qpos, s, NEG_BIG)
        m_blk = jnp.max(s, axis=0, keepdims=True)
        if first:
            m_new = m_blk
        else:
            m_new = jnp.maximum(m_scr[...], m_blk)
        e = jnp.exp2(s * scale2 - m_new * scale2)
        l_blk = jnp.sum(e, axis=0, keepdims=True)
        o_blk = mm(vt_scr[j], e.astype(BF))
        if first:
            l_scr[...] = l_blk
            acc_scr[...] = o_blk
        else:
            alpha = jnp.exp2((m_scr[...] - m_new) * scale2)
            l_scr[...] = l_scr[...] * alpha + l_blk
            acc_scr[...] = acc_scr[...] * alpha + o_blk
        m_scr[...] = m_new

    update(i, True, True)

    def body(j, _):
        update(j, False, False)
        return _

    lax.fori_loop(0, i, body, 0)
    ot = acc_scr[...] / l_scr[...]
    o_ref[...] = ot.T.astype(BF)
    dot_t = do_ref[...].astype(F32).T
    dd_ref[...] = jnp.sum(dot_t * ot, axis=0, keepdims=True)
    lse_ref[...] = m_scr[...] * scale2 + jnp.log2(l_scr[...])


def bwd_kernel(blk, nb, dn, dv, q_ref, do_ref, lse_ref, dd_ref, kc_ref, v_ref, kt_ref, c_ref, wuk_ref, wuv_ref,
               dq_ref, dc_ref, dr_ref, dwk_ref, dwv_ref, dqt_scr, dk_scr, dv_scr):
    step = pl.program_id(0)
    j = nb - 1 - step
    qk = q_ref.shape[1]
    scale = qk ** -0.5
    scale2 = scale * LOG2E
    kc = kc_ref[...]
    v = v_ref[...]
    kt = kt_ref[0]

    def pair(i, masked, first):
        qs = pl.ds(pl.multiple_of(i * blk, blk), blk)
        q = q_ref[qs, :]
        do = do_ref[qs, :]
        s = mm_nt(kc, q)
        p = jnp.exp2(s * scale2 - lse_ref[:, qs])
        if masked:
            kpos = lax.broadcasted_iota(jnp.int32, (blk, blk), 0)
            qpos = lax.broadcasted_iota(jnp.int32, (blk, blk), 1)
            p = jnp.where(kpos <= qpos, p, 0.0)
        dp = mm_nt(v, do)
        ds = (p * (dp - dd_ref[:, qs])).astype(BF)
        dq_blk = mm(kt, ds)
        dk_blk = mm(ds, q)
        dv_blk = mm(p.astype(BF), do)
        if first:
            dqt_scr[i] = dq_blk
            dk_scr[...] = dk_blk
            dv_scr[...] = dv_blk
        else:
            dqt_scr[i] += dq_blk
            dk_scr[...] += dk_blk
            dv_scr[...] += dv_blk

    pair(j, True, True)

    def body(i, _):
        pair(i, False, False)
        return _

    lax.fori_loop(j + 1, nb, body, 0)
    dk = dk_scr[...] * scale
    dkb = dk[:, :dn].astype(BF)
    dvb = dv_scr[...].astype(BF)
    dr_ref[...] = dk[:, dn:]
    dc_ref[...] = mm_nt(dkb, wuk_ref[...]) + mm_nt(dvb, wuv_ref[...])
    dwk = mm_tn(c_ref[...], dkb)
    dwv = mm_tn(c_ref[...], dvb)

    @pl.when(step == 0)
    def _():
        dwk_ref[...] = dwk
        dwv_ref[...] = dwv

    @pl.when(step > 0)
    def _():
        dwk_ref[...] += dwk
        dwv_ref[...] += dwv

    @pl.when(step == nb - 1)
    def _():
        def fin(i, _):
            qs = pl.ds(pl.multiple_of(i * blk, blk), blk)
            dq_ref[qs, :] = (dqt_scr[i] * scale).T
            return _
        lax.fori_loop(0, nb, fin, 0)


def attention(c, r, q, do, wuk, wuv, blk=512, vmem=60 * 2**20):
    t, rank = c.shape
    dr = r.shape[1]
    qk = q.shape[1]
    dn = wuk.shape[1]
    dv = wuv.shape[1]
    nb = t // blk
    row = lambda i: (i, 0)
    col = lambda i: (0, i)
    full = lambda i: (0, 0)
    sds = jax.ShapeDtypeStruct
    o, lse, dd, kc, v, kt = pl.pallas_call(
        functools.partial(fwd_kernel, blk, dn, dv),
        grid=(nb,),
        in_specs=[pl.BlockSpec((blk, rank), row), pl.BlockSpec((blk, dr), row), pl.BlockSpec((blk, qk), row),
                  pl.BlockSpec((blk, dv), row), pl.BlockSpec((rank, dn), full), pl.BlockSpec((rank, dv), full)],
        out_specs=[pl.BlockSpec((blk, dv), row), pl.BlockSpec((1, blk), col), pl.BlockSpec((1, blk), col),
                   pl.BlockSpec((blk, qk), row), pl.BlockSpec((blk, dv), row),
                   pl.BlockSpec((1, qk, blk), lambda i: (i, 0, 0))],
        out_shape=[sds((t, dv), BF), sds((1, t), F32), sds((1, t), F32), sds((t, qk), BF), sds((t, dv), BF),
                   sds((nb, qk, blk), BF)],
        scratch_shapes=[pltpu.VMEM((nb, dv, blk), BF), pltpu.VMEM((t, qk), BF), pltpu.VMEM((1, blk), F32),
                        pltpu.VMEM((1, blk), F32), pltpu.VMEM((dv, blk), F32)],
        compiler_params=pltpu.CompilerParams(vmem_limit_bytes=vmem),
        name="mla_fwd",
    )(c, r, q, do, wuk, wuv)
    rrow = lambda s: (nb - 1 - s, 0)
    dq, dc, drk, dwk, dwv = pl.pallas_call(
        functools.partial(bwd_kernel, blk, nb, dn, dv),
        grid=(nb,),
        in_specs=[pl.BlockSpec((t, qk), full), pl.BlockSpec((t, dv), full), pl.BlockSpec((1, t), full),
                  pl.BlockSpec((1, t), full), pl.BlockSpec((blk, qk), rrow), pl.BlockSpec((blk, dv), rrow),
                  pl.BlockSpec((1, qk, blk), lambda s: (nb - 1 - s, 0, 0)), pl.BlockSpec((blk, rank), rrow),
                  pl.BlockSpec((rank, dn), full), pl.BlockSpec((rank, dv), full)],
        out_specs=[pl.BlockSpec((t, qk), full), pl.BlockSpec((blk, rank), rrow), pl.BlockSpec((blk, dr), rrow),
                   pl.BlockSpec((rank, dn), full), pl.BlockSpec((rank, dv), full)],
        out_shape=[sds((t, qk), F32), sds((t, rank), F32), sds((t, dr), F32), sds((rank, dn), F32), sds((rank, dv), F32)],
        scratch_shapes=[pltpu.VMEM((nb, qk, blk), F32), pltpu.VMEM((blk, qk), F32), pltpu.VMEM((blk, dv), F32)],
        compiler_params=pltpu.CompilerParams(vmem_limit_bytes=vmem),
        name="mla_bwd",
    )(q, do, lse, dd, kc, v, kt, c, wuk, wuv)
    return o, dq, dc, drk, dwk, dwv


PIECE = 1024
LANES = 128


def ar_kernel(strides, side, dc_ref, dr_ref, dco_ref, dro_ref, acc, d2d, *scr):
    rbufs, (loc_sem, send_sem, recv_sem) = scr[:-3], scr[-3:]
    tp = lax.axis_index("tp")
    cp = lax.axis_index("cp")
    n_half = 2
    cols = dco_ref.shape[1] // LANES
    n_units = n_half * cols + 1
    coord = [lax.rem(tp // st, side) for st in strides]

    def nbr(a, off):
        return tp + (lax.rem(coord[a] + off + side, side) - coord[a]) * strides[a]

    barrier = pltpu.get_barrier_semaphore()
    for a in range(3):
        for off in (1, side - 1):
            pl.semaphore_signal(barrier, inc=1, device_id={"tp": nbr(a, off)}, device_id_type=pl.DeviceIdType.MESH)
    pl.semaphore_signal(barrier, inc=1, device_id={"cp": 1 - cp}, device_id_type=pl.DeviceIdType.MESH)
    pl.semaphore_wait(barrier, 7)

    def part(u, owner):
        if u == n_units - 1:
            return dr_ref.at[owner]
        w, b = divmod(u, cols)
        piece = owner if w == 0 else 3 - owner
        return dc_ref.at[pl.ds(pl.multiple_of(piece * PIECE, PIECE), PIECE), pl.ds(b * LANES, LANES)]

    def out_at(u, start, n):
        if u == n_units - 1:
            return dro_ref.at[pl.ds(start, n), :]
        w, b = divmod(u, cols)
        return dco_ref.at[pl.ds(pl.multiple_of(w * PIECE + start, 8), n), pl.ds(b * LANES, LANES)]

    sends = []

    def copy(src, dst, u, k, dev):
        cpy = pltpu.make_async_remote_copy(src_ref=src, dst_ref=dst, send_sem=send_sem.at[u, k], recv_sem=recv_sem.at[u, k],
                                           device_id=dev, device_id_type=pl.DeviceIdType.MESH)
        cpy.start()
        sends.append(cpy)
        return cpy

    first = []
    for u in range(n_units):
        far = copy(part(u, 1 - cp), d2d.at[u], u, 0, {"cp": 1 - cp})
        near = pltpu.make_async_copy(part(u, cp), acc.at[u], loc_sem.at[u])
        near.start()
        first.append((near, far))

    def unit(u):
        axes = [(u + t) % 3 for t in range(3)]
        near, far = first[u]
        near.wait()
        far.wait_recv()
        acc[u] = acc[u] + d2d[u]
        k = 1
        base, size = 0, PIECE
        levels = []
        for t, a in enumerate(axes):
            n = size // side
            h = n // 2
            i = coord[a]
            r1, r2 = rbufs[2 * t], rbufs[2 * t + 1]
            at = lambda o, extra=0: pl.multiple_of(base + lax.rem(i + o, side) * n + extra, 8)
            fwd, bwd = {"tp": nbr(a, 1)}, {"tp": nbr(a, side - 1)}
            opp = at(2)
            c1 = copy(acc.at[u, pl.ds(opp, h)], r1.at[u, 0], u, k, fwd)
            c2 = copy(acc.at[u, pl.ds(at(2, h), h)], r1.at[u, 1], u, k + 1, bwd)
            yield
            c1.wait_recv()
            p1 = at(1)
            acc[u, pl.ds(p1, h)] = acc[u, pl.ds(p1, h)] + r1[u, 0]
            c3 = copy(acc.at[u, pl.ds(p1, n)], r2.at[u, 0], u, k + 2, fwd)
            c2.wait_recv()
            m1 = at(side - 1)
            m1h = at(side - 1, h)
            acc[u, pl.ds(m1h, h)] = acc[u, pl.ds(m1h, h)] + r1[u, 1]
            c4 = copy(acc.at[u, pl.ds(m1, n)], r2.at[u, 1], u, k + 3, bwd)
            yield
            c3.wait_recv()
            c4.wait_recv()
            own = at(0)
            total = acc[u, pl.ds(own, n)] + r2[u, 0] + r2[u, 1]
            if t < 2:
                acc[u, pl.ds(own, n)] = total
            else:
                out_at(u, own, n)[...] = total
            levels.append((base, n, a))
            base, size = own, n
            k += 4
        for base, n, a in reversed(levels):
            h = n // 2
            i = coord[a]
            at = lambda o, extra=0: pl.multiple_of(base + lax.rem(i + o, side) * n + extra, 8)
            fwd, bwd = {"tp": nbr(a, 1)}, {"tp": nbr(a, side - 1)}
            mine = out_at(u, at(0), n)
            c1 = copy(mine, mine, u, k, fwd)
            c2 = copy(mine, mine, u, k + 1, bwd)
            yield
            c1.wait_recv()
            got = out_at(u, at(side - 1), h)
            c3 = copy(got, got, u, k + 2, fwd)
            c2.wait_recv()
            got = out_at(u, at(1, h), h)
            c4 = copy(got, got, u, k + 3, bwd)
            yield
            c3.wait_recv()
            c4.wait_recv()
            k += 4

    live = [unit(u) for u in range(n_units)]
    while live:
        nxt = []
        for g in live:
            try:
                next(g)
                nxt.append(g)
            except StopIteration:
                pass
        live = nxt
    for c in sends:
        c.wait_send()


def all_reduce(dc, drp, side=4, vmem=60 * 2**20):
    rows = dc.shape[0] // 2
    cols = dc.shape[1] // LANES
    nu = 2 * cols + 1
    bufs = []
    size = PIECE
    for _ in range(3):
        n = size // side
        bufs += [pltpu.VMEM((nu, 2, n // 2, LANES), F32), pltpu.VMEM((nu, 2, n, LANES), F32)]
        size = n
    return pl.pallas_call(
        functools.partial(ar_kernel, (1, side, side * side), side),
        in_specs=[pl.BlockSpec(memory_space=pl.ANY)] * 2,
        out_specs=[pl.BlockSpec(memory_space=pltpu.VMEM)] * 2,
        out_shape=[jax.ShapeDtypeStruct((rows, dc.shape[1]), F32), jax.ShapeDtypeStruct((PIECE, LANES), F32)],
        scratch_shapes=[pltpu.VMEM((nu, PIECE, LANES), F32), pltpu.VMEM((nu, PIECE, LANES), F32)] + bufs
        + [pltpu.SemaphoreType.DMA((nu,)), pltpu.SemaphoreType.DMA((nu, 25)), pltpu.SemaphoreType.DMA((nu, 25))],
        compiler_params=pltpu.CompilerParams(collective_id=0, has_side_effects=True, vmem_limit_bytes=vmem),
        name="grad_sum",
    )(dc, drp)


def solution(mesh):
    n_cp = mesh.shape['cp']
    side = round(mesh.shape['tp'] ** (1 / 3))
    swap = [(d, n_cp - 1 - d) for d in range(n_cp)]
    seq_spec = P(('dp', 'cp'), None)
    head_spec = P(('dp', 'cp'), 'tp', None)
    weight_spec = P(None, 'tp', None)
    grad_spec = P('dp', 'tp', None)

    def device_fn(c_latent, k_rope, q_heads, d_out, w_uk, w_uv):
        me = lax.axis_index('cp')
        other = 1 - me
        half = c_latent.shape[0] // 2
        pick = lambda x, h: lax.dynamic_index_in_dim(x, h, 1, keepdims=False)
        xchg = lambda x: lax.ppermute(x, 'cp', swap)

        def natural(own, far):
            outer = jnp.where(me == 0, own, far)
            inner = jnp.where(me == 0, far, own)
            return jnp.concatenate([outer[:half], inner, outer[half:]], axis=0)

        def unnatural(full):
            outer = jnp.concatenate([full[:half], full[3 * half:]], axis=0)
            inner = full[half:3 * half]
            return jnp.where(me == 0, outer, inner), jnp.where(me == 0, inner, outer)

        c = natural(c_latent, xchg(c_latent))
        r = natural(k_rope, xchg(k_rope))
        q = natural(pick(q_heads, me), xchg(pick(q_heads, other)))
        do = natural(pick(d_out, me), xchg(pick(d_out, other)))
        o, dq, dc, dr, dwk, dwv = attention(c, r, q, do, pick(w_uk, me), pick(w_uv, me))
        drp = jnp.stack([jnp.concatenate([dr[:half], dr[3 * half:]], axis=1),
                         jnp.concatenate([dr[half:2 * half], dr[2 * half:3 * half]], axis=1)])
        dc_sum, drp_sum = all_reduce(dc, drp, side)
        dr_sum = jnp.concatenate([drp_sum[:, :64], drp_sum[:, 64:]], axis=0)

        def pair(own, far):
            return jnp.where(me == 0, jnp.stack([own, far], axis=1), jnp.stack([far, own], axis=1))

        o_own, o_far = unnatural(o)
        dq_own, dq_far = unnatural(dq)
        return (pair(o_own, xchg(o_far)), pair(dq_own, xchg(dq_far)), dc_sum, dr_sum,
                pair(dwk, xchg(dwk)), pair(dwv, xchg(dwv)))

    return jax.shard_map(device_fn, mesh=mesh,
                         in_specs=(seq_spec, seq_spec, head_spec, head_spec, weight_spec, weight_spec),
                         out_specs=(head_spec, head_spec, seq_spec, seq_spec, grad_spec, grad_spec),
                         check_vma=False)
```

```python
import functools
import math
import jax
import jax.numpy as jnp
from jax import lax
from jax.experimental import pallas as pl
from jax.experimental.pallas import tpu as pltpu
from jax.sharding import PartitionSpec as P
BF = jnp.bfloat16
F32 = jnp.float32
NEG_BIG = -1.0e30
LOG2E = math.log2(math.e)
LANES = 128
BLK = 512
MESH = pl.DeviceIdType.MESH


def mm(a, b):
    return lax.dot_general(a, b, (((1,), (0,)), ((), ())), preferred_element_type=F32)


def mm_nt(a, b):
    return lax.dot_general(a, b, (((1,), (1,)), ((), ())), preferred_element_type=F32)


def mm_tn(a, b):
    return lax.dot_general(a, b, (((0,), (0,)), ((), ())), preferred_element_type=F32)


def kernel(side, c_in, rt_in, qt_in, do_in, wuk_in, wuv_in,
           o_out, dqt_out, dc_out, drt_out, dwk_out, dwv_out,
           c_scr, rt_scr, qt_scr, dor_scr, wk_scr, wv_scr,
           do_scr, kc_scr, v_scr, kt_scr, vt_scr, o_scr, lse_scr, dd_scr,
           m_scr, l_scr, acc_scr, dqt_scr, dk_scr, dv_scr,
           dcp, drp, dro, dwk_scr, dwv_scr, o_far, dwk_far, dwv_far, d2d,
           ra1, ra2, rb1, rb2, rc1, rc2,
           in_loc, in_snd, in_rcv, x_snd, x_rcv, out_loc, out_snd, out_rcv):
    tp = lax.axis_index("tp")
    me = lax.axis_index("cp")
    strides = (1, side, side * side)
    coord = [lax.rem(tp // st, side) for st in strides]
    nbr = [[tp + (lax.rem(coord[a] + off, side) - coord[a]) * strides[a] for off in (1, side - 1)] for a in range(3)]
    mate = {"cp": 1 - me}
    t_all, rank = c_scr.shape
    piece = t_all // 4
    nb = t_all // BLK
    per = piece // BLK
    qk = qt_scr.shape[0]
    dn = wk_scr.shape[1]
    dr = rt_scr.shape[0]
    scale = qk ** -0.5
    scale2 = scale * LOG2E
    cols = rank // LANES
    n_units = 2 * cols + 1

    def mul(x, n):
        return pl.multiple_of(x, n)

    barrier = pltpu.get_barrier_semaphore()
    for a in range(3):
        for b in range(2):
            pl.semaphore_signal(barrier, inc=1, device_id={"tp": nbr[a][b]}, device_id_type=MESH)
    pl.semaphore_signal(barrier, inc=1, device_id=mate, device_id_type=MESH)
    pl.semaphore_wait(barrier, 7)

    def own_piece(w):
        return jnp.where(w == 0, me, 3 - me) if not isinstance(w, int) else (me if w == 0 else 3 - me)

    def in_refs(w, g, head):
        src = pl.ds(mul(w * piece, piece), piece)
        dst = pl.ds(mul(g * piece, piece), piece)
        return [(c_in.at[src, :], c_scr.at[dst, :]), (rt_in.at[:, src], rt_scr.at[:, dst]),
                (qt_in.at[head, :, src], qt_scr.at[:, dst]), (do_in.at[src], dor_scr.at[dst])]

    def in_local(w, g, k):
        s, d = in_refs(w, g, me)[k]
        return pltpu.make_async_copy(s, d, in_loc.at[k, w])

    def in_remote(w, g, k):
        s, d = in_refs(w, g, 1 - me)[k]
        return pltpu.make_async_remote_copy(src_ref=s, dst_ref=d, send_sem=in_snd.at[k, w], recv_sem=in_rcv.at[k, w],
                                            device_id=mate, device_id_type=MESH)

    for w in range(2):
        for k in range(4):
            in_local(w, own_piece(w), k).start()
            in_remote(w, own_piece(w), k).start()

    wk_scr[...] = jnp.where(me == 0, wuk_in[:, 0, :], wuk_in[:, 1, :])
    wv_scr[...] = jnp.where(me == 0, wuv_in[:, 0, :], wuv_in[:, 1, :])

    kpos = lax.broadcasted_iota(jnp.int32, (BLK, BLK), 0)
    qpos = lax.broadcasted_iota(jnp.int32, (BLK, BLK), 1)

    def blk(i):
        return pl.ds(mul(i * BLK, BLK), BLK)

    def fwd_pair(i, j, masked, first):
        s = mm(kc_scr[blk(j), :], qt_scr[:, blk(i)])
        if masked:
            s = jnp.where(kpos <= qpos, s, NEG_BIG)
        m_blk = jnp.max(s, axis=0, keepdims=True)
        m_new = m_blk if first else jnp.maximum(m_scr[...], m_blk)
        e = jnp.exp2(s * scale2 - m_new * scale2)
        l_blk = jnp.sum(e, axis=0, keepdims=True)
        o_blk = mm(vt_scr[j], e.astype(BF))
        if first:
            l_scr[...] = l_blk
            acc_scr[...] = o_blk
        else:
            alpha = jnp.exp2((m_scr[...] - m_new) * scale2)
            l_scr[...] = l_scr[...] * alpha + l_blk
            acc_scr[...] = acc_scr[...] * alpha + o_blk
        m_scr[...] = m_new

    def fwd_block(i, carry):
        g = i // per
        w = g // 2
        mine = (g == me) | (g == 3 - me)

        @pl.when((lax.rem(i, per) == 0) & mine)
        def _():
            for k in range(4):
                in_local(w, g, k).wait()

        @pl.when((lax.rem(i, per) == 0) & jnp.logical_not(mine))
        def _():
            for k in range(4):
                in_remote(w, g, k).wait_recv()

        rows = blk(i)
        cb = c_scr[rows, :]
        kb = mm(cb, wk_scr[...])
        vb = mm(cb, wv_scr[...])
        rtb = rt_scr[:, rows]
        kc_scr[rows, :dn] = kb.astype(BF)
        kc_scr[rows, dn:] = rtb.astype(F32).T.astype(BF)
        kt_scr[i, :dn, :] = kb.T.astype(BF)
        kt_scr[i, dn:, :] = rtb
        v_scr[rows, :] = vb.astype(BF)
        vt_scr[i] = vb.T.astype(BF)
        x = dor_scr[rows]
        do = jnp.where(me == 0, x[:, 0, :], x[:, 1, :])
        do_scr[rows, :] = do
        fwd_pair(i, i, True, True)

        def body(j, cc):
            fwd_pair(i, j, False, False)
            return cc

        lax.fori_loop(0, i, body, 0)
        ot = acc_scr[...] / l_scr[...]
        o_scr[rows, :] = ot.T.astype(BF)
        dd_scr[:, rows] = jnp.sum(do.astype(F32).T * ot, axis=0, keepdims=True)
        lse_scr[:, rows] = m_scr[...] * scale2 + jnp.log2(l_scr[...])
        return carry

    lax.fori_loop(0, nb, fwd_block, 0)

    def rows_of(u, owner, start, n):
        if u == n_units - 1:
            return drp.at[owner, pl.ds(start, n), :]
        w, b = divmod(u, cols)
        g = owner if w == 0 else 3 - owner
        return dcp.at[pl.ds(mul(g * piece + start, 8), n), pl.ds(b * LANES, LANES)]

    def out_at(u, start, n):
        if u == n_units - 1:
            return dro.at[pl.ds(start, n), :]
        w, b = divmod(u, cols)
        return dc_out.at[pl.ds(mul(w * piece + start, 8), n), pl.ds(b * LANES, LANES)]

    def remote(src, dst, u, k, dev):
        return pltpu.make_async_remote_copy(src_ref=src, dst_ref=dst, send_sem=x_snd.at[u, k], recv_sem=x_rcv.at[u, k],
                                            device_id=dev, device_id_type=MESH)

    rbufs = ((ra1, ra2), (rb1, rb2), (rc1, rc2))

    def make_stages(u):
        axes = [(u + t) % 3 for t in range(3)]
        rows_u = piece
        far = lambda: remote(rows_of(u, 1 - me, 0, rows_u), d2d.at[u], u, 0, mate)
        own = lambda s, n: rows_of(u, me, s, n)
        levels = []
        base, size = 0, rows_u
        for t, a in enumerate(axes):
            n = size // side
            levels.append((base, n, a, t))
            base, size = base + coord[a] * n, n

        def spot(lv, off, extra=0):
            base, n, a, t = lv
            return mul(base + lax.rem(coord[a] + off, side) * n + extra, 8)

        def rs_copies(lv):
            base, n, a, t = lv
            h = n // 2
            fwd, bwd = {"tp": nbr[a][0]}, {"tp": nbr[a][1]}
            r1, r2 = rbufs[t]
            k = 1 + 4 * t
            return [lambda: remote(own(spot(lv, 2), h), r1.at[u, 0], u, k, fwd),
                    lambda: remote(own(spot(lv, 2, h), h), r1.at[u, 1], u, k + 1, bwd),
                    lambda: remote(own(spot(lv, 1), n), r2.at[u, 0], u, k + 2, fwd),
                    lambda: remote(own(spot(lv, side - 1), n), r2.at[u, 1], u, k + 3, bwd)]

        def ag_copies(lv):
            base, n, a, t = lv
            h = n // 2
            fwd, bwd = {"tp": nbr[a][0]}, {"tp": nbr[a][1]}
            k = 13 + 4 * t
            def same(s, m, kk, dev):
                r = out_at(u, s, m)
                return remote(r, r, u, kk, dev)
            return [lambda: same(spot(lv, 0), n, k, fwd), lambda: same(spot(lv, 0), n, k + 1, bwd),
                    lambda: same(spot(lv, side - 1), h, k + 2, fwd), lambda: same(spot(lv, 1, h), h, k + 3, bwd)]

        rs = [rs_copies(lv) for lv in levels]
        ag = [ag_copies(lv) for lv in levels]
        copies = [far] + [c for g in rs for c in g] + [c for g in ag for c in g]
        stages = []

        def s_start():
            far().start()

        def s_near():
            far().wait_recv()
            r = own(0, rows_u)
            r[...] = r[...] + d2d[u]
            rs[0][0]().start()
            rs[0][1]().start()

        stages += [s_start, s_near]
        for t in range(3):
            def s_mid(t=t):
                lv = levels[t]
                h = lv[1] // 2
                r1 = rbufs[t][0]
                rs[t][0]().wait_recv()
                p = own(spot(lv, 1), h)
                p[...] = p[...] + r1[u, 0]
                rs[t][2]().start()
                rs[t][1]().wait_recv()
                p = own(spot(lv, side - 1, h), h)
                p[...] = p[...] + r1[u, 1]
                rs[t][3]().start()

            def s_end(t=t):
                lv = levels[t]
                n = lv[1]
                r2 = rbufs[t][1]
                rs[t][2]().wait_recv()
                rs[t][3]().wait_recv()
                p = own(spot(lv, 0), n)
                total = p[...] + r2[u, 0] + r2[u, 1]
                if t < 2:
                    p[...] = total
                    rs[t + 1][0]().start()
                    rs[t + 1][1]().start()
                else:
                    out_at(u, spot(lv, 0), n)[...] = total
                    ag[2][0]().start()
                    ag[2][1]().start()

            stages += [s_mid, s_end]
        for t in (2, 1, 0):
            def s_fwd(t=t):
                ag[t][0]().wait_recv()
                ag[t][2]().start()
                ag[t][1]().wait_recv()
                ag[t][3]().start()

            def s_got(t=t):
                ag[t][2]().wait_recv()
                ag[t][3]().wait_recv()
                if t > 0:
                    ag[t - 1][0]().start()
                    ag[t - 1][1]().start()

            stages += [s_fwd, s_got]
        return stages, copies

    plans = [make_stages(u) for u in range(n_units)]
    n_stage = len(plans[0][0])
    early = list(range(cols, 2 * cols))
    late = list(range(0, cols)) + [n_units - 1]

    def run_stage(k, units):
        for u in units:
            plans[u][0][k]()

    hooks = [11, 12, 14, 16, 18, 20, 22, 24, 26, 29, 30, 32, 34]

    def bwd_block(step, carry):
        j = nb - 1 - step
        t0 = step * (step + 1) // 2
        bwd_diag(j)

        def body(i, cc):
            t = t0 + (i - j)
            for k, tk in enumerate(hooks):
                @pl.when(t == tk)
                def _(k=k):
                    run_stage(k, early)
            bwd_off(j, i)
            return cc

        lax.fori_loop(j + 1, nb, body, 0)
        rows = blk(j)
        dk = dk_scr[...] * scale
        dkb = dk[:, :dn].astype(BF)
        dvb = dv_scr[...].astype(BF)
        dcp[rows, :] = mm_nt(dkb, wk_scr[...]) + mm_nt(dvb, wv_scr[...])
        drt = dk[:, dn:].T
        g = j // per
        owner = jnp.where((g == 0) | (g == 3), 0, 1)
        lt0 = (g // 2) * (piece // LANES) + lax.rem(j, per) * (BLK // LANES)
        for rt in range(dr // 8):
            for lt in range(BLK // LANES):
                row = mul((rt * (2 * piece // LANES) + lt0 + lt) * 8, 8)
                drp[owner, pl.ds(row, 8), :] = drt[rt * 8:rt * 8 + 8, lt * LANES:(lt + 1) * LANES]
        dwk = mm_tn(c_scr[rows, :], dkb)
        dwv = mm_tn(c_scr[rows, :], dvb)

        @pl.when(step == 0)
        def _():
            dwk_scr[...] = dwk
            dwv_scr[...] = dwv

        @pl.when(step > 0)
        def _():
            dwk_scr[...] += dwk
            dwv_scr[...] += dwv

        return carry

    def bwd_core(j, i, masked, first):
        q = qt_scr[:, blk(i)]
        do = do_scr[blk(i), :]
        s = mm(kc_scr[blk(j), :], q)
        p = jnp.exp2(s * scale2 - lse_scr[:, blk(i)])
        if masked:
            p = jnp.where(kpos <= qpos, p, 0.0)
        dp = mm_nt(v_scr[blk(j), :], do)
        ds = (p * (dp - dd_scr[:, blk(i)])).astype(BF)
        dq_blk = mm(kt_scr[j], ds)
        dk_blk = mm_nt(ds, q)
        dv_blk = mm(p.astype(BF), do)
        if first:
            dk_scr[...] = dk_blk
            dv_scr[...] = dv_blk
            dqt_scr[i] = dq_blk
        else:
            dk_scr[...] += dk_blk
            dv_scr[...] += dv_blk
            dqt_scr[i] += dq_blk

    def bwd_diag(j):
        bwd_core(j, j, True, True)

    def bwd_off(j, i):
        bwd_core(j, i, False, False)

    lax.fori_loop(0, nb, bwd_block, 0)

    run_stage(0, late)
    run_stage(n_stage - 1, early)

    def x_o(w):
        g = own_piece(w)
        far_g = (1 - me) if w == 0 else 2 + me
        return pltpu.make_async_remote_copy(src_ref=o_scr.at[pl.ds(mul(far_g * piece, piece), piece), :],
                                            dst_ref=o_far.at[pl.ds(w * piece, piece), :],
                                            send_sem=out_snd.at[w], recv_sem=out_rcv.at[w],
                                            device_id=mate, device_id_type=MESH)

    def x_w(k):
        s, d = ((dwk_scr, dwk_far), (dwv_scr, dwv_far))[k]
        return pltpu.make_async_remote_copy(src_ref=s, dst_ref=d, send_sem=out_snd.at[2 + k], recv_sem=out_rcv.at[2 + k],
                                            device_id=mate, device_id_type=MESH)

    def x_q(w, b):
        far_g = (1 - me) if w == 0 else 2 + me
        return pltpu.make_async_remote_copy(src_ref=dqt_scr.at[far_g * per + b],
                                            dst_ref=dqt_out.at[me, :, pl.ds((w * per + b) * BLK, BLK)],
                                            send_sem=out_snd.at[4 + w * per + b], recv_sem=out_rcv.at[4 + w * per + b],
                                            device_id=mate, device_id_type=MESH)

    for w in range(2):
        x_o(w).start()
    for k in range(2):
        x_w(k).start()
    for i in range(nb):
        dqt_scr[i] = dqt_scr[i] * scale
    for w in range(2):
        for b in range(per):
            x_q(w, b).start()
    run_stage(1, late)
    for w in range(2):
        for b in range(per):
            dqt_out[me, :, pl.ds((w * per + b) * BLK, BLK)] = dqt_scr[own_piece(w) * per + b]
    run_stage(2, late)
    for w in range(2):
        x_o(w).wait_recv()
        mine = o_scr[pl.ds(mul(own_piece(w) * piece, piece), piece), :]
        other = o_far[pl.ds(w * piece, piece), :]
        o_out[pl.ds(w * piece, piece), 0, :] = jnp.where(me == 0, mine, other)
        o_out[pl.ds(w * piece, piece), 1, :] = jnp.where(me == 0, other, mine)
    run_stage(3, late)
    for k, (s, f, o) in enumerate(((dwk_scr, dwk_far, dwk_out), (dwv_scr, dwv_far, dwv_out))):
        x_w(k).wait_recv()
        o[:, 0, :] = jnp.where(me == 0, s[...], f[...])
        o[:, 1, :] = jnp.where(me == 0, f[...], s[...])
    for k in range(4, n_stage):
        run_stage(k, late)
    for rt in range(dr // 8):
        for lt in range(2 * piece // LANES):
            row = (rt * (2 * piece // LANES) + lt) * 8
            drt_out[rt * 8:rt * 8 + 8, lt * LANES:(lt + 1) * LANES] = dro[row:row + 8, :]
    for w in range(2):
        for b in range(per):
            x_q(w, b).wait()
        x_o(w).wait_send()
        x_w(w).wait_send()
        for k in range(4):
            in_remote(w, own_piece(w), k).wait_send()
    for u in range(n_units):
        for cpy in plans[u][1]:
            cpy().wait_send()


def run(c, rt, qt, do, wuk, wuv, side, vmem=60 * 2**20):
    half, rank = c.shape
    t = 2 * half
    dr = rt.shape[0]
    qk = qt.shape[1]
    dn = wuk.shape[2]
    dv = wuv.shape[2]
    nb = t // BLK
    piece = t // 4
    nu = 2 * (rank // LANES) + 1
    sds = jax.ShapeDtypeStruct
    vm = pltpu.VMEM
    bufs = []
    size = piece
    for _ in range(3):
        n = size // side
        bufs += [vm((nu, 2, n // 2, LANES), F32), vm((nu, 2, n, LANES), F32)]
        size = n
    dma = pltpu.SemaphoreType.DMA
    any_spec = pl.BlockSpec(memory_space=pl.ANY)
    vm_spec = pl.BlockSpec(memory_space=pltpu.VMEM)
    return pl.pallas_call(
        functools.partial(kernel, side),
        in_specs=[any_spec] * 4 + [vm_spec] * 2,
        out_specs=[vm_spec] * 6,
        out_shape=[sds((half, 2, dv), BF), sds((2, qk, half), F32), sds((half, rank), F32), sds((dr, half), F32),
                   sds((rank, 2, dn), F32), sds((rank, 2, dv), F32)],
        scratch_shapes=[vm((t, rank), BF), vm((dr, t), BF), vm((qk, t), BF), vm((t, 2, dv), BF), vm((rank, dn), BF), vm((rank, dv), BF),
                        vm((t, dv), BF), vm((t, qk), BF), vm((t, dv), BF), vm((nb, qk, BLK), BF), vm((nb, dv, BLK), BF),
                        vm((t, dv), BF), vm((1, t), F32), vm((1, t), F32),
                        vm((1, BLK), F32), vm((1, BLK), F32), vm((dv, BLK), F32), vm((nb, qk, BLK), F32),
                        vm((BLK, qk), F32), vm((BLK, dv), F32),
                        vm((t, rank), F32), vm((2, piece, LANES), F32), vm((piece, LANES), F32), vm((rank, dn), F32), vm((rank, dv), F32),
                        vm((half, dv), BF), vm((rank, dn), F32), vm((rank, dv), F32), vm((nu, piece, LANES), F32)]
        + bufs + [dma((4, 2)), dma((4, 2)), dma((4, 2)), dma((nu, 25)), dma((nu, 25)), dma((1,)), dma((8,)), dma((8,))],
        compiler_params=pltpu.CompilerParams(collective_id=0, has_side_effects=True, vmem_limit_bytes=vmem),
        name="mla_step",
    )(c, rt, qt, do, wuk, wuv)


def solution(mesh):
    side = round(mesh.shape['tp'] ** (1 / 3))
    seq_spec = P(('dp', 'cp'), None)
    head_spec = P(('dp', 'cp'), 'tp', None)
    weight_spec = P(None, 'tp', None)
    grad_spec = P('dp', 'tp', None)

    def device_fn(c_latent, k_rope, q_heads, d_out, w_uk, w_uv):
        o, dqt, dc, drt, dwk, dwv = run(c_latent, k_rope.T, jnp.transpose(q_heads, (1, 2, 0)), d_out, w_uk, w_uv, side)
        return o, jnp.transpose(dqt, (2, 0, 1)), dc, drt.T, dwk, dwv

    return jax.shard_map(device_fn, mesh=mesh,
                         in_specs=(seq_spec, seq_spec, head_spec, head_spec, weight_spec, weight_spec),
                         out_specs=(head_spec, head_spec, seq_spec, seq_spec, grad_spec, grad_spec),
                         check_vma=False)
```

```python
import functools
import math
import jax
import jax.numpy as jnp
from jax import lax
from jax.experimental import pallas as pl
from jax.experimental.pallas import tpu as pltpu
from jax.sharding import PartitionSpec as P
BF = jnp.bfloat16
F32 = jnp.float32
NEG_BIG = -1.0e30
LOG2E = math.log2(math.e)
LANES = 128
BLK = 512
MESH = pl.DeviceIdType.MESH


def mm(a, b):
    return lax.dot_general(a, b, (((1,), (0,)), ((), ())), preferred_element_type=F32)


def mm_nt(a, b):
    return lax.dot_general(a, b, (((1,), (1,)), ((), ())), preferred_element_type=F32)


def mm_tn(a, b):
    return lax.dot_general(a, b, (((0,), (0,)), ((), ())), preferred_element_type=F32)


def kernel(side, c_in, rt_in, qt_in, do_in, wuk_in, wuv_in,
           o_out, dqt_out, dc_out, drt_out, dwk_out, dwv_out,
           c_scr, rt_scr, qt_scr, dor_scr, wk_scr, wv_scr,
           do_scr, kc_scr, v_scr, kt_scr, vt_scr, o_scr, lse_scr, dd_scr,
           m_scr, l_scr, acc_scr, dqt_scr, dk_scr, dv_scr,
           wide16_scr, wide_scr, dcp, drp, dro, dwk_scr, dwv_scr, o_far, dwk_far, dwv_far, d2d,
           ra1, ra2, rb1, rb2, rc1, rc2,
           in_loc, in_snd, in_rcv, x_snd, x_rcv, out_loc, out_snd, out_rcv):
    tp = lax.axis_index("tp")
    me = lax.axis_index("cp")
    strides = (1, side, side * side)
    coord = [lax.rem(tp // st, side) for st in strides]
    nbr = [[tp + (lax.rem(coord[a] + off, side) - coord[a]) * strides[a] for off in (1, side - 1)] for a in range(3)]
    mate = {"cp": 1 - me}
    t_all, rank = c_scr.shape
    piece = t_all // 4
    nb = t_all // BLK
    per = piece // BLK
    qk = qt_scr.shape[0]
    dn = wk_scr.shape[1]
    dr = rt_scr.shape[0]
    scale = qk ** -0.5
    scale2 = scale * LOG2E
    cols = rank // LANES
    n_units = 2 * cols + 1

    def mul(x, n):
        return pl.multiple_of(x, n)

    barrier = pltpu.get_barrier_semaphore()
    for a in range(3):
        for b in range(2):
            pl.semaphore_signal(barrier, inc=1, device_id={"tp": nbr[a][b]}, device_id_type=MESH)
    pl.semaphore_signal(barrier, inc=1, device_id=mate, device_id_type=MESH)
    pl.semaphore_wait(barrier, 7)

    def own_piece(w):
        return jnp.where(w == 0, me, 3 - me) if not isinstance(w, int) else (me if w == 0 else 3 - me)

    def in_refs(w, g, head):
        src = pl.ds(mul(w * piece, piece), piece)
        dst = pl.ds(mul(g * piece, piece), piece)
        return [(c_in.at[src, :], c_scr.at[dst, :]), (rt_in.at[:, src], rt_scr.at[:, dst]),
                (qt_in.at[head, :, src], qt_scr.at[:, dst]), (do_in.at[src], dor_scr.at[dst])]

    def in_local(w, g, k):
        s, d = in_refs(w, g, me)[k]
        return pltpu.make_async_copy(s, d, in_loc.at[k, w])

    def in_remote(w, g, k):
        s, d = in_refs(w, g, 1 - me)[k]
        return pltpu.make_async_remote_copy(src_ref=s, dst_ref=d, send_sem=in_snd.at[k, w], recv_sem=in_rcv.at[k, w],
                                            device_id=mate, device_id_type=MESH)

    for w in range(2):
        for k in range(4):
            in_local(w, own_piece(w), k).start()
            in_remote(w, own_piece(w), k).start()

    def unpack(x):
        x = x.reshape(x.shape[0], 2 * x.shape[2])
        d = x.shape[1] // 2
        return jnp.where(me == 0, x[:, :d], x[:, d:])

    def pack(buf, mine, other):
        d = mine.shape[1]
        buf[:, :d] = jnp.where(me == 0, mine, other)
        buf[:, d:] = jnp.where(me == 0, other, mine)
        return buf[...].reshape(buf.shape[0], 2, d)

    wk_scr[...] = unpack(wuk_in[...])
    wv_scr[...] = unpack(wuv_in[...])

    kpos = lax.broadcasted_iota(jnp.int32, (BLK, BLK), 0)
    qpos = lax.broadcasted_iota(jnp.int32, (BLK, BLK), 1)

    def blk(i):
        return pl.ds(mul(i * BLK, BLK), BLK)

    def fwd_pair(i, j, masked, first):
        s = mm(kc_scr[blk(j), :], qt_scr[:, blk(i)])
        if masked:
            s = jnp.where(kpos <= qpos, s, NEG_BIG)
        m_blk = jnp.max(s, axis=0, keepdims=True)
        m_new = m_blk if first else jnp.maximum(m_scr[...], m_blk)
        e = jnp.exp2(s * scale2 - m_new * scale2)
        l_blk = jnp.sum(e, axis=0, keepdims=True)
        o_blk = mm(vt_scr[j], e.astype(BF))
        if first:
            l_scr[...] = l_blk
            acc_scr[...] = o_blk
        else:
            alpha = jnp.exp2((m_scr[...] - m_new) * scale2)
            l_scr[...] = l_scr[...] * alpha + l_blk
            acc_scr[...] = acc_scr[...] * alpha + o_blk
        m_scr[...] = m_new

    def fwd_block(i, carry):
        g = i // per
        w = g // 2
        mine = (g == me) | (g == 3 - me)

        @pl.when((lax.rem(i, per) == 0) & mine)
        def _():
            for k in range(4):
                in_local(w, g, k).wait()

        @pl.when((lax.rem(i, per) == 0) & jnp.logical_not(mine))
        def _():
            for k in range(4):
                in_remote(w, g, k).wait_recv()

        rows = blk(i)
        cb = c_scr[rows, :]
        kb = mm(cb, wk_scr[...])
        vb = mm(cb, wv_scr[...])
        rtb = rt_scr[:, rows]
        kc_scr[rows, :dn] = kb.astype(BF)
        kc_scr[rows, dn:] = rtb.astype(F32).T.astype(BF)
        kt_scr[i, :dn, :] = kb.T.astype(BF)
        kt_scr[i, dn:, :] = rtb
        v_scr[rows, :] = vb.astype(BF)
        vt_scr[i] = vb.T.astype(BF)
        do = unpack(dor_scr[rows])
        do_scr[rows, :] = do
        fwd_pair(i, i, True, True)

        def body(j, cc):
            fwd_pair(i, j, False, False)
            return cc

        lax.fori_loop(0, i, body, 0)
        ot = acc_scr[...] / l_scr[...]
        o_scr[rows, :] = ot.T.astype(BF)
        dd_scr[:, rows] = jnp.sum(do.astype(F32).T * ot, axis=0, keepdims=True)
        lse_scr[:, rows] = m_scr[...] * scale2 + jnp.log2(l_scr[...])
        return carry

    lax.fori_loop(0, nb, fwd_block, 0)

    def rows_of(u, owner, start, n):
        if u == n_units - 1:
            return drp.at[owner, pl.ds(start, n), :]
        w, b = divmod(u, cols)
        g = owner if w == 0 else 3 - owner
        return dcp.at[pl.ds(mul(g * piece + start, 8), n), pl.ds(b * LANES, LANES)]

    def out_at(u, start, n):
        if u == n_units - 1:
            return dro.at[pl.ds(start, n), :]
        w, b = divmod(u, cols)
        return dc_out.at[pl.ds(mul(w * piece + start, 8), n), pl.ds(b * LANES, LANES)]

    def remote(src, dst, u, k, dev):
        return pltpu.make_async_remote_copy(src_ref=src, dst_ref=dst, send_sem=x_snd.at[u, k], recv_sem=x_rcv.at[u, k],
                                            device_id=dev, device_id_type=MESH)

    rbufs = ((ra1, ra2), (rb1, rb2), (rc1, rc2))

    def make_stages(u):
        axes = [(u + t) % 3 for t in range(3)]
        rows_u = piece
        far = lambda: remote(rows_of(u, 1 - me, 0, rows_u), d2d.at[u], u, 0, mate)
        own = lambda s, n: rows_of(u, me, s, n)
        levels = []
        base, size = 0, rows_u
        for t, a in enumerate(axes):
            n = size // side
            levels.append((base, n, a, t))
            base, size = base + coord[a] * n, n

        def spot(lv, off, extra=0):
            base, n, a, t = lv
            return mul(base + lax.rem(coord[a] + off, side) * n + extra, 8)

        def rs_copies(lv):
            base, n, a, t = lv
            h = n // 2
            fwd, bwd = {"tp": nbr[a][0]}, {"tp": nbr[a][1]}
            r1, r2 = rbufs[t]
            k = 1 + 4 * t
            return [lambda: remote(own(spot(lv, 2), h), r1.at[u, 0], u, k, fwd),
                    lambda: remote(own(spot(lv, 2, h), h), r1.at[u, 1], u, k + 1, bwd),
                    lambda: remote(own(spot(lv, 1), n), r2.at[u, 0], u, k + 2, fwd),
                    lambda: remote(own(spot(lv, side - 1), n), r2.at[u, 1], u, k + 3, bwd)]

        def ag_copies(lv):
            base, n, a, t = lv
            h = n // 2
            fwd, bwd = {"tp": nbr[a][0]}, {"tp": nbr[a][1]}
            k = 13 + 4 * t
            def same(s, m, kk, dev):
                r = out_at(u, s, m)
                return remote(r, r, u, kk, dev)
            return [lambda: same(spot(lv, 0), n, k, fwd), lambda: same(spot(lv, 0), n, k + 1, bwd),
                    lambda: same(spot(lv, side - 1), h, k + 2, fwd), lambda: same(spot(lv, 1, h), h, k + 3, bwd)]

        rs = [rs_copies(lv) for lv in levels]
        ag = [ag_copies(lv) for lv in levels]
        copies = [far] + [c for g in rs for c in g] + [c for g in ag for c in g]
        stages = []

        def s_start():
            far().start()

        def s_near():
            far().wait_recv()
            r = own(0, rows_u)
            r[...] = r[...] + d2d[u]
            rs[0][0]().start()
            rs[0][1]().start()

        stages += [s_start, s_near]
        for t in range(3):
            def s_mid(t=t):
                lv = levels[t]
                h = lv[1] // 2
                r1 = rbufs[t][0]
                rs[t][0]().wait_recv()
                p = own(spot(lv, 1), h)
                p[...] = p[...] + r1[u, 0]
                rs[t][2]().start()
                rs[t][1]().wait_recv()
                p = own(spot(lv, side - 1, h), h)
                p[...] = p[...] + r1[u, 1]
                rs[t][3]().start()

            def s_end(t=t):
                lv = levels[t]
                n = lv[1]
                r2 = rbufs[t][1]
                rs[t][2]().wait_recv()
                rs[t][3]().wait_recv()
                p = own(spot(lv, 0), n)
                total = p[...] + r2[u, 0] + r2[u, 1]
                if t < 2:
                    p[...] = total
                    rs[t + 1][0]().start()
                    rs[t + 1][1]().start()
                else:
                    out_at(u, spot(lv, 0), n)[...] = total
                    ag[2][0]().start()
                    ag[2][1]().start()

            stages += [s_mid, s_end]
        for t in (2, 1, 0):
            def s_fwd(t=t):
                ag[t][0]().wait_recv()
                ag[t][2]().start()
                ag[t][1]().wait_recv()
                ag[t][3]().start()

            def s_got(t=t):
                ag[t][2]().wait_recv()
                ag[t][3]().wait_recv()
                if t > 0:
                    ag[t - 1][0]().start()
                    ag[t - 1][1]().start()

            stages += [s_fwd, s_got]
        return stages, copies

    plans = [make_stages(u) for u in range(n_units)]
    n_stage = len(plans[0][0])
    early = list(range(cols, 2 * cols))
    late = list(range(0, cols)) + [n_units - 1]

    def run_stage(k, units):
        for u in units:
            plans[u][0][k]()

    hooks = [11, 12, 14, 16, 18, 20, 22, 24, 26, 29, 30, 32, 34]

    def bwd_block(step, carry):
        j = nb - 1 - step
        t0 = step * (step + 1) // 2
        bwd_diag(j)

        def body(i, cc):
            t = t0 + (i - j)
            for k, tk in enumerate(hooks):
                @pl.when(t == tk)
                def _(k=k):
                    run_stage(k, early)
            bwd_off(j, i)
            return cc

        lax.fori_loop(j + 1, nb, body, 0)
        rows = blk(j)
        dk = dk_scr[...] * scale
        dkb = dk[:, :dn].astype(BF)
        dvb = dv_scr[...].astype(BF)
        dcp[rows, :] = mm_nt(dkb, wk_scr[...]) + mm_nt(dvb, wv_scr[...])
        drt = dk[:, dn:].T
        g = j // per
        owner = jnp.where((g == 0) | (g == 3), 0, 1)
        lt0 = (g // 2) * (piece // LANES) + lax.rem(j, per) * (BLK // LANES)
        for rt in range(dr // 8):
            for lt in range(BLK // LANES):
                row = mul((rt * (2 * piece // LANES) + lt0 + lt) * 8, 8)
                drp[owner, pl.ds(row, 8), :] = drt[rt * 8:rt * 8 + 8, lt * LANES:(lt + 1) * LANES]
        dwk = mm_tn(c_scr[rows, :], dkb)
        dwv = mm_tn(c_scr[rows, :], dvb)

        @pl.when(step == 0)
        def _():
            dwk_scr[...] = dwk
            dwv_scr[...] = dwv

        @pl.when(step > 0)
        def _():
            dwk_scr[...] += dwk
            dwv_scr[...] += dwv

        return carry

    def bwd_core(j, i, masked, first):
        q = qt_scr[:, blk(i)]
        do = do_scr[blk(i), :]
        s = mm(kc_scr[blk(j), :], q)
        p = jnp.exp2(s * scale2 - lse_scr[:, blk(i)])
        if masked:
            p = jnp.where(kpos <= qpos, p, 0.0)
        dp = mm_nt(v_scr[blk(j), :], do)
        ds = (p * (dp - dd_scr[:, blk(i)])).astype(BF)
        dq_blk = mm(kt_scr[j], ds)
        dk_blk = mm_nt(ds, q)
        dv_blk = mm(p.astype(BF), do)
        if first:
            dk_scr[...] = dk_blk
            dv_scr[...] = dv_blk
            dqt_scr[i] = dq_blk
        else:
            dk_scr[...] += dk_blk
            dv_scr[...] += dv_blk
            dqt_scr[i] += dq_blk

    def bwd_diag(j):
        bwd_core(j, j, True, True)

    def bwd_off(j, i):
        bwd_core(j, i, False, False)

    lax.fori_loop(0, nb, bwd_block, 0)

    run_stage(0, late)
    run_stage(n_stage - 1, early)

    def x_o(w):
        g = own_piece(w)
        far_g = (1 - me) if w == 0 else 2 + me
        return pltpu.make_async_remote_copy(src_ref=o_scr.at[pl.ds(mul(far_g * piece, piece), piece), :],
                                            dst_ref=o_far.at[pl.ds(w * piece, piece), :],
                                            send_sem=out_snd.at[w], recv_sem=out_rcv.at[w],
                                            device_id=mate, device_id_type=MESH)

    def x_w(k):
        s, d = ((dwk_scr, dwk_far), (dwv_scr, dwv_far))[k]
        return pltpu.make_async_remote_copy(src_ref=s, dst_ref=d, send_sem=out_snd.at[2 + k], recv_sem=out_rcv.at[2 + k],
                                            device_id=mate, device_id_type=MESH)

    def x_q(w, b):
        far_g = (1 - me) if w == 0 else 2 + me
        return pltpu.make_async_remote_copy(src_ref=dqt_scr.at[far_g * per + b],
                                            dst_ref=dqt_out.at[me, :, pl.ds((w * per + b) * BLK, BLK)],
                                            send_sem=out_snd.at[4 + w * per + b], recv_sem=out_rcv.at[4 + w * per + b],
                                            device_id=mate, device_id_type=MESH)

    for w in range(2):
        x_o(w).start()
    for k in range(2):
        x_w(k).start()
    for i in range(nb):
        dqt_scr[i] = dqt_scr[i] * scale
    for w in range(2):
        for b in range(per):
            x_q(w, b).start()
    run_stage(1, late)
    for w in range(2):
        for b in range(per):
            dqt_out[me, :, pl.ds((w * per + b) * BLK, BLK)] = dqt_scr[own_piece(w) * per + b]
    run_stage(2, late)
    for w in range(2):
        x_o(w).wait_recv()
        mine = o_scr[pl.ds(mul(own_piece(w) * piece, piece), piece), :]
        other = o_far[pl.ds(w * piece, piece), :]
        o_out[pl.ds(w * piece, piece)] = pack(wide16_scr, mine, other)
    run_stage(3, late)
    for k, (s, f, o) in enumerate(((dwk_scr, dwk_far, dwk_out), (dwv_scr, dwv_far, dwv_out))):
        x_w(k).wait_recv()
        o[...] = pack(wide_scr, s[...], f[...])
    for k in range(4, n_stage):
        run_stage(k, late)
    for rt in range(dr // 8):
        for lt in range(2 * piece // LANES):
            row = (rt * (2 * piece // LANES) + lt) * 8
            drt_out[rt * 8:rt * 8 + 8, lt * LANES:(lt + 1) * LANES] = dro[row:row + 8, :]
    for w in range(2):
        for b in range(per):
            x_q(w, b).wait()
        x_o(w).wait_send()
        x_w(w).wait_send()
        for k in range(4):
            in_remote(w, own_piece(w), k).wait_send()
    for u in range(n_units):
        for cpy in plans[u][1]:
            cpy().wait_send()


def run(c, rt, qt, do, wuk, wuv, side, vmem=52 * 2**20):
    half, rank = c.shape
    t = 2 * half
    dr = rt.shape[0]
    qk = qt.shape[1]
    dn = wuk.shape[2]
    dv = wuv.shape[2]
    nb = t // BLK
    piece = t // 4
    nu = 2 * (rank // LANES) + 1
    sds = jax.ShapeDtypeStruct
    vm = pltpu.VMEM
    bufs = []
    size = piece
    for _ in range(3):
        n = size // side
        bufs += [vm((nu, 2, n // 2, LANES), F32), vm((nu, 2, n, LANES), F32)]
        size = n
    dma = pltpu.SemaphoreType.DMA
    any_spec = pl.BlockSpec(memory_space=pl.ANY)
    vm_spec = pl.BlockSpec(memory_space=pltpu.VMEM)
    return pl.pallas_call(
        functools.partial(kernel, side),
        in_specs=[any_spec] * 4 + [vm_spec] * 2,
        out_specs=[vm_spec] * 6,
        out_shape=[vm((half, 2, dv), BF), vm((2, qk, half), F32), vm((half, rank), F32), vm((dr, half), F32),
                   vm((rank, 2, dn), F32), vm((rank, 2, dv), F32)],
        scratch_shapes=[vm((t, rank), BF), vm((dr, t), BF), vm((qk, t), BF), vm((t, 2, dv), BF), vm((rank, dn), BF), vm((rank, dv), BF),
                        vm((t, dv), BF), vm((t, qk), BF), vm((t, dv), BF), vm((nb, qk, BLK), BF), vm((nb, dv, BLK), BF),
                        vm((t, dv), BF), vm((1, t), F32), vm((1, t), F32),
                        vm((1, BLK), F32), vm((1, BLK), F32), vm((dv, BLK), F32), vm((nb, qk, BLK), F32),
                        vm((BLK, qk), F32), vm((BLK, dv), F32), vm((piece, 2 * dv), BF), vm((rank, 2 * dn), F32),
                        vm((t, rank), F32), vm((2, piece, LANES), F32), vm((piece, LANES), F32), vm((rank, dn), F32), vm((rank, dv), F32),
                        vm((half, dv), BF), vm((rank, dn), F32), vm((rank, dv), F32), vm((nu, piece, LANES), F32)]
        + bufs + [dma((4, 2)), dma((4, 2)), dma((4, 2)), dma((nu, 25)), dma((nu, 25)), dma((1,)), dma((8,)), dma((8,))],
        compiler_params=pltpu.CompilerParams(collective_id=0, has_side_effects=True, vmem_limit_bytes=vmem),
        name="mla_step",
    )(c, rt, qt, do, wuk, wuv)


def solution(mesh):
    side = round(mesh.shape['tp'] ** (1 / 3))
    seq_spec = P(('dp', 'cp'), None)
    head_spec = P(('dp', 'cp'), 'tp', None)
    weight_spec = P(None, 'tp', None)
    grad_spec = P('dp', 'tp', None)

    def device_fn(c_latent, k_rope, q_heads, d_out, w_uk, w_uv):
        o, dqt, dc, drt, dwk, dwv = run(c_latent, k_rope.T, jnp.transpose(q_heads, (1, 2, 0)), d_out, w_uk, w_uv, side)
        return o, jnp.transpose(dqt, (2, 0, 1)), dc, drt.T, dwk, dwv

    return jax.shard_map(device_fn, mesh=mesh,
                         in_specs=(seq_spec, seq_spec, head_spec, head_spec, weight_spec, weight_spec),
                         out_specs=(head_spec, head_spec, seq_spec, seq_spec, grad_spec, grad_spec),
                         check_vma=False)
```

```python
import functools
import math
import jax
import jax.numpy as jnp
from jax import lax
from jax.experimental import pallas as pl
from jax.experimental.pallas import tpu as pltpu
from jax.sharding import PartitionSpec as P
BF = jnp.bfloat16
F32 = jnp.float32
NEG_BIG = -1.0e30
LOG2E = math.log2(math.e)
LANES = 128
BLK = 512
HOOKS_A = (0, 3, 6, 9, 10, 12, 13)
HOOKS_B = (7, 8, 10, 12, 13)
MESH = pl.DeviceIdType.MESH


def mm(a, b):
    return lax.dot_general(a, b, (((1,), (0,)), ((), ())), preferred_element_type=F32)


def mm_nt(a, b):
    return lax.dot_general(a, b, (((1,), (1,)), ((), ())), preferred_element_type=F32)


def mm_tn(a, b):
    return lax.dot_general(a, b, (((0,), (0,)), ((), ())), preferred_element_type=F32)


def kernel(side, c_in, rt_in, qt_in, do_in, wuk_in, wuv_in,
           o_out, dqt_out, sum_out, drt_out, dwk_out, dwv_out,
           c_scr, rt_scr, qt_scr, dor_scr, wk_scr, wv_scr,
           do_scr, kc_scr, v_scr, kt_scr, vt_scr, o_scr, lse_scr, dd_scr,
           m_scr, l_scr, acc_scr, dqt_scr, dk_scr, dv_scr,
           dkv_scr, wide_scr, dcp, dwk_scr, dwv_scr, o_far, dwk_far, dwv_far, d2d,
           ra1, ra2, rb1, rb2, rc1, rc2,
           in_loc, in_snd, in_rcv, x_snd, x_rcv, out_loc, out_snd, out_rcv):
    tp = lax.axis_index("tp")
    me = lax.axis_index("cp")
    strides = (1, side, side * side)
    coord = [lax.rem(tp // st, side) for st in strides]
    nbr = [[tp + (lax.rem(coord[a] + off, side) - coord[a]) * strides[a] for off in (1, side - 1)] for a in range(3)]
    mate = {"cp": 1 - me}
    t_all, rank = c_scr.shape
    piece = t_all // 4
    nb = t_all // BLK
    per = piece // BLK
    qk = qt_scr.shape[0]
    dn = wk_scr.shape[1]
    dr = rt_scr.shape[0]
    scale = qk ** -0.5
    scale2 = scale * LOG2E
    cols = rank // LANES

    def mul(x, n):
        return pl.multiple_of(x, n)

    barrier = pltpu.get_barrier_semaphore()
    for a in range(3):
        for b in range(2):
            pl.semaphore_signal(barrier, inc=1, device_id={"tp": nbr[a][b]}, device_id_type=MESH)
    pl.semaphore_signal(barrier, inc=1, device_id=mate, device_id_type=MESH)
    pl.semaphore_wait(barrier, 7)

    def own_piece(w):
        return jnp.where(w == 0, me, 3 - me) if not isinstance(w, int) else (me if w == 0 else 3 - me)

    def in_refs(w, g, head):
        src = pl.ds(mul(w * piece, piece), piece)
        dst = pl.ds(mul(g * piece, piece), piece)
        return [(c_in.at[src, :], c_scr.at[dst, :]), (rt_in.at[:, src], rt_scr.at[:, dst]),
                (qt_in.at[head, :, src], qt_scr.at[:, dst]), (do_in.at[src], dor_scr.at[dst])]

    def in_local(w, g, k):
        s, d = in_refs(w, g, me)[k]
        return pltpu.make_async_copy(s, d, in_loc.at[k, w])

    def in_remote(w, g, k):
        s, d = in_refs(w, g, 1 - me)[k]
        return pltpu.make_async_remote_copy(src_ref=s, dst_ref=d, send_sem=in_snd.at[k, w], recv_sem=in_rcv.at[k, w],
                                            device_id=mate, device_id_type=MESH)

    for w in range(2):
        for k in range(4):
            in_local(w, own_piece(w), k).start()
            in_remote(w, own_piece(w), k).start()

    def unpack(x):
        x = x.reshape(x.shape[0], 2 * x.shape[2])
        d = x.shape[1] // 2
        return jnp.where(me == 0, x[:, :d], x[:, d:])

    def pack(buf, mine, other):
        d = mine.shape[1]
        buf[:, :d] = jnp.where(me == 0, mine, other)
        buf[:, d:] = jnp.where(me == 0, other, mine)
        return buf[...].reshape(buf.shape[0], 2, d)

    wk_scr[...] = unpack(wuk_in[...])
    wv_scr[...] = unpack(wuv_in[...])

    def blk(i):
        return pl.ds(mul(i * BLK, BLK), BLK)

    def lo(n):
        return pl.ds(0, n)

    def soft_update(s, vt, cols, first):
        m_blk = jnp.max(s, axis=0, keepdims=True)
        m_new = m_blk if first else jnp.maximum(m_scr[:, cols], m_blk)
        e = jnp.exp2(s * scale2 - m_new * scale2)
        l_blk = jnp.sum(e, axis=0, keepdims=True)
        o_blk = mm(vt, e.astype(BF))
        if first:
            l_scr[:, cols] = l_blk
            acc_scr[:, cols] = o_blk
        else:
            alpha = jnp.exp2((m_scr[:, cols] - m_new) * scale2)
            l_scr[:, cols] = l_scr[:, cols] * alpha + l_blk
            acc_scr[:, cols] = acc_scr[:, cols] * alpha + o_blk
        m_scr[:, cols] = m_new

    def cut(n_k, n_q):
        kp = lax.broadcasted_iota(jnp.int32, (n_k, n_q), 0)
        qp = lax.broadcasted_iota(jnp.int32, (n_k, n_q), 1)
        return kp <= qp

    def fwd_piece(g, carry):
        w = g // 2
        mine = (g == me) | (g == 3 - me)

        @pl.when(mine)
        def _():
            for k in range(4):
                in_local(w, g, k).wait()

        @pl.when(jnp.logical_not(mine))
        def _():
            for k in range(4):
                in_remote(w, g, k).wait_recv()

        rows = pl.ds(mul(g * piece, piece), piece)
        cb = c_scr[rows, :]
        kb = mm(cb, wk_scr[...])
        vb = mm(cb, wv_scr[...])
        rtb = rt_scr[:, rows]
        kc_scr[rows, :dn] = kb.astype(BF)
        kc_scr[rows, dn:] = rtb.astype(F32).T.astype(BF)
        kt_scr[g, :dn, :] = kb.T.astype(BF)
        kt_scr[g, dn:, :] = rtb
        v_scr[rows, :] = vb.astype(BF)
        vt_scr[g] = vb.T.astype(BF)
        do = unpack(dor_scr[rows])
        do_scr[rows, :] = do
        qt = qt_scr[:, rows]
        low = pl.ds(mul(g * piece, piece), BLK)
        high = pl.ds(mul(g * piece + BLK, BLK), BLK)
        s = mm(kc_scr[low, :], qt)
        soft_update(jnp.where(cut(BLK, piece), s, NEG_BIG), vt_scr[g, :, :BLK], slice(None), True)
        s = mm(kc_scr[high, :], qt_scr[:, high])
        soft_update(jnp.where(cut(BLK, BLK), s, NEG_BIG), vt_scr[g, :, BLK:], slice(BLK, piece), False)

        def body(j, cc):
            fwd_full(g, j)
            return cc

        lax.fori_loop(0, g, body, 0)
        ot = acc_scr[...] / l_scr[...]
        o_scr[rows, :] = ot.T.astype(BF)
        dd_scr[:, rows] = jnp.sum(do.astype(F32).T * ot, axis=0, keepdims=True)
        lse_scr[:, rows] = m_scr[...] * scale2 + jnp.log2(l_scr[...])
        return carry

    ra, rb, cs = 128, 256, BLK

    def fwd_full(g, j):
        mx, st = {}, {}
        bufs = (dcp.at[:piece, :], dcp.at[piece:2 * piece, :])

        def score(c, r):
            s = mm(kc_scr[pl.ds(mul(j * piece + r * ra, ra), ra), :], qt_scr[:, pl.ds(mul(g * piece + c * cs, cs), cs)])
            bufs[c % 2][r * ra:(r + 1) * ra, :] = s
            p = jnp.max(s, axis=0, keepdims=True)
            mx[c] = p if c not in mx else jnp.maximum(mx[c], p)

        def mid(c):
            cols = slice(c * cs, (c + 1) * cs)
            m_old = m_scr[:, cols]
            m_new = jnp.maximum(m_old, mx[c])
            m_scr[:, cols] = m_new
            st[c] = [m_new * scale2, jnp.exp2((m_old - m_new) * scale2), None, None]

        def weigh(c, r):
            d = st[c]
            e = jnp.exp2(bufs[c % 2][r * rb:(r + 1) * rb, :] * scale2 - d[0])
            p = jnp.sum(e, axis=0, keepdims=True)
            o = mm(vt_scr[j, :, r * rb:(r + 1) * rb], e.astype(BF))
            d[2] = p if d[2] is None else d[2] + p
            d[3] = o if d[3] is None else d[3] + o

        def fin(c):
            cols = slice(c * cs, (c + 1) * cs)
            d = st[c]
            l_scr[:, cols] = l_scr[:, cols] * d[1] + d[2]
            acc_scr[:, cols] = acc_scr[:, cols] * d[1] + d[3]

        na, nr = piece // ra, piece // rb
        for r in range(na):
            score(0, r)
        for c in range(piece // cs):
            mid(c)
            for r in range(na):
                if c + 1 < piece // cs:
                    score(c + 1, r)
                if r % (na // nr) == na // nr - 1:
                    weigh(c, r // (na // nr))
            fin(c)

    lax.fori_loop(0, 4, fwd_piece, 0)

    rbufs = ((ra1, ra2), (rb1, rb2), (rc1, rc2))
    sets = {"a": ((2, cols, 0), (3, cols, 1)), "b": ((1, cols, 0),), "c": ((0, cols, 0), (4, 2, 1))}

    def pick(a, xs):
        return jnp.where(a == 0, xs[0], jnp.where(a == 1, xs[1], xs[2]))

    class Unit:
        def __init__(self, wh, b, turn):
            self.wh, self.b = wh, b
            self.u = wh * cols + b
            self.lanes = pl.ds(mul(b * LANES, LANES), LANES)
            first = lax.rem(b + turn, 3)
            self.level = []
            base, size = 0, BLK
            for t in range(3):
                a = lax.rem(first + t, 3)
                n = size // side
                here = pick(a, coord)
                self.level.append((base, n, here, pick(a, [x[0] for x in nbr]), pick(a, [x[1] for x in nbr])))
                base, size = base + here * n, n

        def part(self, owner, start, n):
            if self.wh == 4:
                top = t_all + owner * BLK
            else:
                top = (owner if self.wh < 2 else 3 - owner) * piece + (self.wh % 2) * BLK
            return dcp.at[pl.ds(mul(top + start, 8), n), self.lanes]

        def own(self, start, n):
            return self.part(me, start, n)

        def out(self, start, n):
            return sum_out.at[pl.ds(mul(self.wh * BLK + start, 8), n), self.lanes]

        def spot(self, t, off, extra=0):
            base, n, here, _, _ = self.level[t]
            return base + lax.rem(here + off, side) * n + extra

        def copy(self, src, dst, k, dev):
            return pltpu.make_async_remote_copy(src_ref=src, dst_ref=dst, send_sem=x_snd.at[self.u, k],
                                                recv_sem=x_rcv.at[self.u, k], device_id=dev, device_id_type=MESH)

        def swap(self):
            return self.copy(self.part(1 - me, 0, BLK), d2d.at[self.u], 0, mate)

        def half(self, t):
            n = self.level[t][1]
            return (n // 2, True) if n % 16 == 0 else (n, False)

        def rs(self, t, q):
            _, n, _, fwd, bwd = self.level[t]
            h, _ = self.half(t)
            r1, r2 = rbufs[t]
            src, dst, dev = ((self.spot(t, 2), r1.at[self.u, 0], fwd), (self.spot(t, 2, h), r1.at[self.u, 1], bwd),
                             (self.spot(t, 1), r2.at[self.u, 0], fwd), (self.spot(t, side - 1), r2.at[self.u, 1], bwd))[q]
            return self.copy(self.own(src, h if q < 2 else n), dst, 1 + 4 * t + q, {"tp": dev})

        def ag(self, t, q):
            _, n, _, fwd, bwd = self.level[t]
            h, _ = self.half(t)
            at, m, dev = ((self.spot(t, 0), n, fwd), (self.spot(t, 0), n, bwd),
                          (self.spot(t, side - 1), h, fwd), (self.spot(t, 1, h), h, bwd))[q]
            r = self.out(at, m)
            return self.copy(r, r, 13 + 4 * t + q, {"tp": dev})

        def all_copies(self):
            res = [self.swap()]
            for t in range(3):
                two = self.half(t)[1]
                res += [self.rs(t, q) for q in range(4) if two or q != 1]
                res += [self.ag(t, q) for q in range(4) if two or q != 3]
            return res

        def start_rs(self, t):
            self.rs(t, 0).start()
            if self.half(t)[1]:
                self.rs(t, 1).start()

        def start_ag(self, t):
            self.ag(t, 0).start()
            self.ag(t, 1).start()

        def stage(self, k):
            if k == 0:
                self.swap().start()
            elif k == 1:
                self.swap().wait_recv()
                r = self.own(0, BLK)
                r[...] = r[...] + d2d[self.u]
                self.start_rs(0)
            elif k < 8:
                t, last = divmod(k - 2, 2)
                n = self.level[t][1]
                h, two = self.half(t)
                r1, r2 = rbufs[t]
                if not last:
                    self.rs(t, 0).wait_recv()
                    p = self.own(self.spot(t, 1), h)
                    p[...] = p[...] + r1[self.u, 0]
                    self.rs(t, 2).start()
                    if two:
                        self.rs(t, 1).wait_recv()
                        p = self.own(self.spot(t, side - 1, h), h)
                        p[...] = p[...] + r1[self.u, 1]
                    self.rs(t, 3).start()
                else:
                    self.rs(t, 2).wait_recv()
                    self.rs(t, 3).wait_recv()
                    p = self.own(self.spot(t, 0), n)
                    total = p[...] + r2[self.u, 0] + r2[self.u, 1]
                    if t < 2:
                        p[...] = total
                        self.start_rs(t + 1)
                    else:
                        self.out(self.spot(t, 0), n)[...] = total
                        self.start_ag(2)
            else:
                t, last = divmod(k - 8, 2)
                t = 2 - t
                two = self.half(t)[1]
                if not last:
                    self.ag(t, 0).wait_recv()
                    self.ag(t, 2).start()
                    self.ag(t, 1).wait_recv()
                    if two:
                        self.ag(t, 3).start()
                else:
                    self.ag(t, 2).wait_recv()
                    if two:
                        self.ag(t, 3).wait_recv()
                    if t > 0:
                        self.start_ag(t - 1)

    n_stage = 14

    def each(name, fn):
        for wh, n, turn in sets[name]:
            def body(b, cc, wh=wh, turn=turn):
                fn(Unit(wh, b, turn))
                return cc
            lax.fori_loop(0, n, body, 0)

    def run_stage(k, name):
        each(name, lambda un: un.stage(k))

    plan_a = dict(zip(HOOKS_A, range(len(HOOKS_A))))
    plan_b = dict(zip(HOOKS_B, range(len(HOOKS_B))))

    def hook(t):
        for at in sorted(set(plan_a) | set(plan_b)):
            @pl.when(t == at)
            def _(at=at):
                if at in plan_a:
                    run_stage(plan_a[at], "a")
                if at in plan_b:
                    run_stage(plan_b[at], "b")

    def bwd_core(j, q_rows, kt, mask, first, dq_at):
        q = qt_scr[:, q_rows]
        do = do_scr[q_rows, :]
        s = mm(kc_scr[blk(j), :], q)
        p = jnp.exp2(s * scale2 - lse_scr[:, q_rows])
        if mask is not None:
            p = jnp.where(mask, p, 0.0)
        dp = mm_nt(v_scr[blk(j), :], do)
        ds = (p * (dp - dd_scr[:, q_rows])).astype(BF)
        dq_at[...] += mm(kt, ds)
        dk_blk = mm_nt(ds, q)
        dv_blk = mm(p.astype(BF), do)
        if first:
            dk_scr[...] = dk_blk
            dv_scr[...] = dv_blk
        else:
            dk_scr[...] += dk_blk
            dv_scr[...] += dv_blk

    def bwd_block(step, carry):
        half = step // 4
        s_ = step - 4 * half
        j = 4 * (1 - half) + 3 - 2 * lax.rem(s_, 2) - s_ // 2
        g = j // per
        odd = lax.rem(j, per)
        t0 = 3 * s_ + s_ // 2 - 1000 * (1 - half)
        off = mul(odd * BLK, BLK)

        def body(i, cc):
            hook(t0 + (i - g))

            @pl.when((i == g) & (odd == 1))
            def _():
                high = pl.ds(mul(g * piece + BLK, BLK), BLK)
                bwd_core(j, high, kt_scr[g, :, BLK:], cut(BLK, BLK), True, dqt_scr.at[g, :, BLK:])

            @pl.when((i == g) & (odd == 0))
            def _():
                bwd_core(j, pl.ds(mul(g * piece, piece), piece), kt_scr[g, :, :BLK], cut(BLK, piece), True, dqt_scr.at[g])

            @pl.when(i > g)
            def _():
                bwd_core(j, pl.ds(mul(i * piece, piece), piece), kt_scr[g, :, pl.ds(off, BLK)], None, False, dqt_scr.at[i])

            return cc

        lax.fori_loop(g, 4, body, 0)
        rows = blk(j)
        dk = dk_scr[...] * scale
        dkb = dk[:, :dn].astype(BF)
        dvb = dv_scr[...].astype(BF)
        dkv_scr[rows, :dn] = dkb
        dkv_scr[rows, dn:] = dvb
        dcp[rows, :] = mm_nt(dkb, wk_scr[...]) + mm_nt(dvb, wv_scr[...])
        drt = dk[:, dn:].T
        owner = jnp.where((g == 0) | (g == 3), 0, 1)
        lt0 = (g // 2) * (piece // LANES) + odd * (BLK // LANES)
        lts = 2 * piece // LANES
        for rt in range(dr // 8):
            b, r = divmod(rt * lts * 8, BLK)
            for lt in range(BLK // LANES):
                row = mul(t_all + owner * BLK + r + (lt0 + lt) * 8, 8)
                dcp[pl.ds(row, 8), b * LANES:(b + 1) * LANES] = drt[rt * 8:rt * 8 + 8, lt * LANES:(lt + 1) * LANES]
        return carry

    def d_weights(lo_j, hi_j):
        def body(j, cc):
            rows = blk(j)
            dwk_scr[...] += mm_tn(c_scr[rows, :], dkv_scr[rows, :dn])
            dwv_scr[...] += mm_tn(c_scr[rows, :], dkv_scr[rows, dn:])
            return cc

        lax.fori_loop(lo_j, hi_j, body, 0)

    def x_o(w):
        g = own_piece(w)
        far_g = (1 - me) if w == 0 else 2 + me
        return pltpu.make_async_remote_copy(src_ref=o_scr.at[pl.ds(mul(far_g * piece, piece), piece), :],
                                            dst_ref=o_far.at[pl.ds(w * piece, piece), :],
                                            send_sem=out_snd.at[w], recv_sem=out_rcv.at[w],
                                            device_id=mate, device_id_type=MESH)

    def x_w(k):
        s, d = ((dwk_scr, dwk_far), (dwv_scr, dwv_far))[k]
        return pltpu.make_async_remote_copy(src_ref=s, dst_ref=d, send_sem=out_snd.at[2 + k], recv_sem=out_rcv.at[2 + k],
                                            device_id=mate, device_id_type=MESH)

    def x_q(w):
        far_g = (1 - me) if w == 0 else 2 + me
        return pltpu.make_async_remote_copy(src_ref=dqt_scr.at[far_g], dst_ref=dqt_out.at[me, :, pl.ds(w * piece, piece)],
                                            send_sem=out_snd.at[4 + w], recv_sem=out_rcv.at[4 + w],
                                            device_id=mate, device_id_type=MESH)

    for w in range(2):
        x_o(w).start()
    for g in range(4):
        dqt_scr[g] = jnp.zeros(dqt_scr.shape[1:], F32)
    dwk_scr[...] = jnp.zeros_like(dwk_scr)
    dwv_scr[...] = jnp.zeros_like(dwv_scr)
    lax.fori_loop(0, nb, bwd_block, 0)

    done_a, done_b = len(HOOKS_A), len(HOOKS_B)

    def tail(k):
        run_stage(k, "c")
        if k + done_b < n_stage:
            run_stage(k + done_b, "b")
        if k + done_a < n_stage:
            run_stage(k + done_a, "a")

    tail(0)
    for g in range(4):
        dqt_scr[g] = dqt_scr[g] * scale
    for w in range(2):
        x_q(w).start()
    tail(1)
    d_weights(0, nb // 2)
    tail(2)
    d_weights(nb // 2, nb)
    for k in range(2):
        x_w(k).start()
    tail(3)
    for w in range(2):
        dqt_out[me, :, pl.ds(w * piece, piece)] = dqt_scr[own_piece(w)]
    tail(4)
    for w in range(2):
        x_o(w).wait_recv()
        mine = o_scr[pl.ds(mul(own_piece(w) * piece, piece), piece), :]
        o_out[pl.ds(w * piece, piece)] = pack(dkv_scr.at[pl.ds(0, piece), :], mine, o_far[pl.ds(w * piece, piece), :])
    tail(5)
    for k, (s_, f_, o_) in enumerate(((dwk_scr, dwk_far, dwk_out), (dwv_scr, dwv_far, dwv_out))):
        x_w(k).wait_recv()
        o_[...] = pack(wide_scr, s_[...], f_[...])
    for k in range(6, n_stage):
        tail(k)
    for rt in range(dr // 8):
        for lt in range(2 * piece // LANES):
            b, r = divmod((rt * (2 * piece // LANES) + lt) * 8, BLK)
            r += 2 * piece
            drt_out[rt * 8:rt * 8 + 8, lt * LANES:(lt + 1) * LANES] = sum_out[r:r + 8, b * LANES:(b + 1) * LANES]
    for w in range(2):
        x_q(w).wait()
        x_o(w).wait_send()
        x_w(w).wait_send()
        for k in range(4):
            in_remote(w, own_piece(w), k).wait_send()

    def drain(un):
        for cpy in un.all_copies():
            cpy.wait_send()

    for name in sets:
        each(name, drain)


def run(c, rt, qt, do, wuk, wuv, side, vmem=51 * 2**20):
    half, rank = c.shape
    t = 2 * half
    dr = rt.shape[0]
    qk = qt.shape[1]
    dn = wuk.shape[2]
    dv = wuv.shape[2]
    nb = t // BLK
    piece = t // 4
    nu = 4 * (rank // LANES) + 2
    sds = jax.ShapeDtypeStruct
    vm = pltpu.VMEM
    bufs = []
    size = BLK
    for _ in range(3):
        n = size // side
        h = n // 2 if n % 16 == 0 else n
        bufs += [vm((nu, 2, h, LANES), F32), vm((nu, 2, n, LANES), F32)]
        size = n
    dma = pltpu.SemaphoreType.DMA
    any_spec = pl.BlockSpec(memory_space=pl.ANY)
    vm_spec = pl.BlockSpec(memory_space=pltpu.VMEM)
    return pl.pallas_call(
        functools.partial(kernel, side),
        in_specs=[any_spec] * 4 + [vm_spec] * 2,
        out_specs=[vm_spec] * 6,
        out_shape=[vm((half, 2, dv), BF), vm((2, qk, half), F32), vm((half + BLK, rank), F32), vm((dr, half), F32),
                   vm((rank, 2, dn), F32), vm((rank, 2, dv), F32)],
        scratch_shapes=[vm((t, rank), BF), vm((dr, t), BF), vm((qk, t), BF), vm((t, 2, dv), BF), vm((rank, dn), BF), vm((rank, dv), BF),
                        vm((t, dv), BF), vm((t, qk), BF), vm((t, dv), BF), vm((4, qk, piece), BF), vm((4, dv, piece), BF),
                        vm((t, dv), BF), vm((1, t), F32), vm((1, t), F32),
                        vm((1, piece), F32), vm((1, piece), F32), vm((dv, piece), F32), vm((4, qk, piece), F32),
                        vm((BLK, qk), F32), vm((BLK, dv), F32), vm((t, dn + dv), BF), vm((rank, 2 * dn), F32),
                        vm((t + 2 * BLK, rank), F32), vm((rank, dn), F32), vm((rank, dv), F32),
                        vm((half, dv), BF), vm((rank, dn), F32), vm((rank, dv), F32), vm((nu, BLK, LANES), F32)]
        + bufs + [dma((4, 2)), dma((4, 2)), dma((4, 2)), dma((nu, 25)), dma((nu, 25)), dma((1,)), dma((8,)), dma((8,))],
        compiler_params=pltpu.CompilerParams(collective_id=0, has_side_effects=True, vmem_limit_bytes=vmem),
        name="mla_step",
    )(c, rt, qt, do, wuk, wuv)


def solution(mesh):
    side = round(mesh.shape['tp'] ** (1 / 3))
    seq_spec = P(('dp', 'cp'), None)
    head_spec = P(('dp', 'cp'), 'tp', None)
    weight_spec = P(None, 'tp', None)
    grad_spec = P('dp', 'tp', None)

    def device_fn(c_latent, k_rope, q_heads, d_out, w_uk, w_uv):
        o, dqt, dc, drt, dwk, dwv = run(c_latent, k_rope.T, jnp.transpose(q_heads, (1, 2, 0)), d_out, w_uk, w_uv, side)
        return o, jnp.transpose(dqt, (2, 0, 1)), dc[:c_latent.shape[0]], drt.T, dwk, dwv

    return jax.shard_map(device_fn, mesh=mesh,
                         in_specs=(seq_spec, seq_spec, head_spec, head_spec, weight_spec, weight_spec),
                         out_specs=(head_spec, head_spec, seq_spec, seq_spec, grad_spec, grad_spec),
                         check_vma=False)
```

```python
import functools
import math
import jax
import jax.numpy as jnp
from jax import lax
from jax.experimental import pallas as pl
from jax.experimental.pallas import tpu as pltpu
from jax.sharding import PartitionSpec as P
BF = jnp.bfloat16
F32 = jnp.float32
NEG_BIG = -1.0e30
LOG2E = math.log2(math.e)
LANES = 128
BLK = 512
HOOKS = {2: [(1, "p3", 0)], 5: [(0, "p3", 1)], 8: [(0, "p3", 2)], 10: [(1, "p0", 0)], 11: [(0, "p3", 3)],
         13: [(0, "p3", 4), (0, "p0", 1)], 14: [(0, "p2", 0)], 15: [(0, "p3", 5)], 16: [(0, "p0", 2)],
         17: [(0, "p3", 6), (1, "p2", 1), (0, "p1h", 0)], 19: [(0, "p3", 7), (0, "p0", 3), (1, "p2", 2), (1, "p1h", 1)]}
TAIL = ((0, "p3", 8), (0, "p0", 4), (1, "p2", 3), (1, "p1h", 2), (1, "p1l", 0))
MESH = pl.DeviceIdType.MESH


def mm(a, b):
    return lax.dot_general(a, b, (((1,), (0,)), ((), ())), preferred_element_type=F32)


def mm_nt(a, b):
    return lax.dot_general(a, b, (((1,), (1,)), ((), ())), preferred_element_type=F32)


def mm_tn(a, b):
    return lax.dot_general(a, b, (((0,), (0,)), ((), ())), preferred_element_type=F32)


def kernel(side, c_in, rt_in, qt_in, do_in, wuk_in, wuv_in,
           o_out, dqt_out, sum_out, drt_out, dwk_out, dwv_out,
           c_scr, rt_scr, qt_scr, dor_scr, wkv_scr,
           do_scr, kc_scr, v_scr, kt_scr, vt_scr, o_scr, lse_scr, dd_scr,
           m_scr, l_scr, acc_scr, dqt_scr, dk_scr, dv_scr,
           dkv_scr, wide_scr, dcp, dw_scr, o_far, dw_far, d2d,
           ra1, ra2, rb1, rb2, rc1, rc2,
           in_loc, in_snd, in_rcv, x_snd, x_rcv, out_snd, out_rcv):
    tp = lax.axis_index("tp")
    me = lax.axis_index("cp")
    strides = (1, side, side * side)
    coord = [lax.rem(tp // st, side) for st in strides]
    nbr = [[tp + (lax.rem(coord[a] + off, side) - coord[a]) * strides[a] for off in (1, side - 1)] for a in range(3)]
    mate = {"cp": 1 - me}
    t_all, rank = c_scr.shape
    piece = t_all // 4
    nb = t_all // BLK
    per = piece // BLK
    qk = qt_scr.shape[0]
    dn = dwk_out.shape[2]
    dr = rt_scr.shape[0]
    scale = qk ** -0.5
    scale2 = scale * LOG2E
    cols = rank // LANES

    def mul(x, n):
        return pl.multiple_of(x, n)

    barrier = pltpu.get_barrier_semaphore()
    for a in range(3):
        for b in range(2):
            pl.semaphore_signal(barrier, inc=1, device_id={"tp": nbr[a][b]}, device_id_type=MESH)
    pl.semaphore_signal(barrier, inc=1, device_id=mate, device_id_type=MESH)
    pl.semaphore_wait(barrier, 7)

    def own_piece(w):
        return jnp.where(w == 0, me, 3 - me) if not isinstance(w, int) else (me if w == 0 else 3 - me)

    def in_refs(w, g, head):
        src = pl.ds(mul(w * piece, piece), piece)
        dst = pl.ds(mul(g * piece, piece), piece)
        return [(c_in.at[src, :], c_scr.at[dst, :]), (rt_in.at[:, src], rt_scr.at[:, dst]),
                (qt_in.at[head, :, src], qt_scr.at[:, dst]), (do_in.at[src], dor_scr.at[dst])]

    def in_local(w, g, k):
        s, d = in_refs(w, g, me)[k]
        return pltpu.make_async_copy(s, d, in_loc.at[k, w])

    def in_remote(w, g, k):
        s, d = in_refs(w, g, 1 - me)[k]
        return pltpu.make_async_remote_copy(src_ref=s, dst_ref=d, send_sem=in_snd.at[k, w], recv_sem=in_rcv.at[k, w],
                                            device_id=mate, device_id_type=MESH)

    for w in range(2):
        for k in range(4):
            in_local(w, own_piece(w), k).start()
            in_remote(w, own_piece(w), k).start()

    def unpack(x):
        x = x.reshape(x.shape[0], 2 * x.shape[2])
        d = x.shape[1] // 2
        return jnp.where(me == 0, x[:, :d], x[:, d:])

    def pack(buf, mine, other):
        d = mine.shape[1]
        buf[:, :d] = jnp.where(me == 0, mine, other)
        buf[:, d:] = jnp.where(me == 0, other, mine)
        return buf[...].reshape(buf.shape[0], 2, d)

    wkv_scr[:, :dn] = unpack(wuk_in[...])
    wkv_scr[:, dn:] = unpack(wuv_in[...])

    def blk(i):
        return pl.ds(mul(i * BLK, BLK), BLK)

    def lo(n):
        return pl.ds(0, n)

    def soft_update(s, vt, cols, first):
        m_blk = jnp.max(s, axis=0, keepdims=True)
        m_new = m_blk if first else jnp.maximum(m_scr[:, cols], m_blk)
        e = jnp.exp2(s * scale2 - m_new * scale2)
        l_blk = jnp.sum(e, axis=0, keepdims=True)
        o_blk = mm(vt, e.astype(BF))
        if first:
            l_scr[:, cols] = l_blk
            acc_scr[:, cols] = o_blk
        else:
            alpha = jnp.exp2((m_scr[:, cols] - m_new) * scale2)
            l_scr[:, cols] = l_scr[:, cols] * alpha + l_blk
            acc_scr[:, cols] = acc_scr[:, cols] * alpha + o_blk
        m_scr[:, cols] = m_new

    def cut(n_k, n_q):
        kp = lax.broadcasted_iota(jnp.int32, (n_k, n_q), 0)
        qp = lax.broadcasted_iota(jnp.int32, (n_k, n_q), 1)
        return kp <= qp

    def fwd_piece(g, carry):
        w = g // 2
        mine = (g == me) | (g == 3 - me)

        @pl.when(mine)
        def _():
            for k in range(4):
                in_local(w, g, k).wait()

        @pl.when(jnp.logical_not(mine))
        def _():
            for k in range(4):
                in_remote(w, g, k).wait_recv()

        rows = pl.ds(mul(g * piece, piece), piece)
        cb = c_scr[rows, :]
        kv = mm(cb, wkv_scr[...])
        kb, vb = kv[:, :dn], kv[:, dn:]
        rtb = rt_scr[:, rows]
        kc_scr[rows, :dn] = kb.astype(BF)
        kc_scr[rows, dn:] = rtb.astype(F32).T.astype(BF)
        kt_scr[g, :dn, :] = kb.T.astype(BF)
        kt_scr[g, dn:, :] = rtb
        v_scr[rows, :] = vb.astype(BF)
        vt_scr[g] = vb.T.astype(BF)
        do = unpack(dor_scr[rows])
        do_scr[rows, :] = do
        qt = qt_scr[:, rows]
        low = pl.ds(mul(g * piece, piece), BLK)
        high = pl.ds(mul(g * piece + BLK, BLK), BLK)
        s = mm(kc_scr[low, :], qt)
        soft_update(jnp.where(cut(BLK, piece), s, NEG_BIG), vt_scr[g, :, :BLK], slice(None), True)
        s = mm(kc_scr[high, :], qt_scr[:, high])
        soft_update(jnp.where(cut(BLK, BLK), s, NEG_BIG), vt_scr[g, :, BLK:], slice(BLK, piece), False)

        def body(j, cc):
            fwd_full(g, j)
            return cc

        lax.fori_loop(0, g, body, 0)
        ot = acc_scr[...] / l_scr[...]
        o_scr[rows, :] = ot.T.astype(BF)
        dd_scr[:, rows] = jnp.sum(do.astype(F32).T * ot, axis=0, keepdims=True)
        lse_scr[:, rows] = m_scr[...] * scale2 + jnp.log2(l_scr[...])
        return carry

    ra, rb, cs = 128, 256, BLK

    def fwd_full(g, j):
        mx, st = {}, {}
        bufs = (dcp.at[:piece, :], dcp.at[piece:2 * piece, :])

        def score(c, r):
            s = mm(kc_scr[pl.ds(mul(j * piece + r * ra, ra), ra), :], qt_scr[:, pl.ds(mul(g * piece + c * cs, cs), cs)])
            bufs[c % 2][r * ra:(r + 1) * ra, :] = s
            p = jnp.max(s, axis=0, keepdims=True)
            mx[c] = p if c not in mx else jnp.maximum(mx[c], p)

        def mid(c):
            cols = slice(c * cs, (c + 1) * cs)
            m_old = m_scr[:, cols]
            m_new = jnp.maximum(m_old, mx[c])
            m_scr[:, cols] = m_new
            st[c] = [m_new * scale2, jnp.exp2((m_old - m_new) * scale2), None, None]

        def weigh(c, r):
            d = st[c]
            e = jnp.exp2(bufs[c % 2][r * rb:(r + 1) * rb, :] * scale2 - d[0])
            p = jnp.sum(e, axis=0, keepdims=True)
            o = mm(vt_scr[j, :, r * rb:(r + 1) * rb], e.astype(BF))
            d[2] = p if d[2] is None else d[2] + p
            d[3] = o if d[3] is None else d[3] + o

        def fin(c):
            cols = slice(c * cs, (c + 1) * cs)
            d = st[c]
            l_scr[:, cols] = l_scr[:, cols] * d[1] + d[2]
            acc_scr[:, cols] = acc_scr[:, cols] * d[1] + d[3]

        na, nr = piece // ra, piece // rb
        for r in range(na):
            score(0, r)
        for c in range(piece // cs):
            mid(c)
            for r in range(na):
                if c + 1 < piece // cs:
                    score(c + 1, r)
                if r % (na // nr) == na // nr - 1:
                    weigh(c, r // (na // nr))
            fin(c)

    lax.fori_loop(0, 4, fwd_piece, 0)

    rbufs = ((ra1, ra2), (rb1, rb2), (rc1, rc2))
    sets = {"p3": ((2, cols, 0), (3, cols, 1)), "p0": ((0, cols, 0), (1, cols, 1), (4, 2, 0)),
            "p2": ((2, cols, 0), (3, cols, 1)), "p1h": ((1, cols, 0),), "p1l": ((0, cols, 0), (4, 2, 1))}

    def pick(a, xs):
        return jnp.where(a == 0, xs[0], jnp.where(a == 1, xs[1], xs[2]))

    class Unit:
        def __init__(self, wh, b, turn):
            self.wh, self.b = wh, b
            self.u = wh * cols + b
            self.lanes = pl.ds(mul(b * LANES, LANES), LANES)
            first = lax.rem(b + turn, 3)
            self.level = []
            base, size = 0, BLK
            for t in range(3):
                a = lax.rem(first + t, 3)
                n = size // side
                here = pick(a, coord)
                self.level.append((base, n, here, pick(a, [x[0] for x in nbr]), pick(a, [x[1] for x in nbr])))
                base, size = base + here * n, n

        def part(self, owner, start, n):
            if self.wh == 4:
                top = t_all + owner * BLK
            else:
                top = (owner if self.wh < 2 else 3 - owner) * piece + (self.wh % 2) * BLK
            return dcp.at[pl.ds(mul(top + start, 8), n), self.lanes]

        def own(self, start, n):
            return self.part(me, start, n)

        def out(self, start, n):
            return sum_out.at[pl.ds(mul(self.wh * BLK + start, 8), n), self.lanes]

        def spot(self, t, off, extra=0):
            base, n, here, _, _ = self.level[t]
            return base + lax.rem(here + off, side) * n + extra

        def copy(self, src, dst, k, dev, slot):
            return pltpu.make_async_remote_copy(src_ref=src, dst_ref=dst, send_sem=x_snd.at[self.u, slot],
                                                recv_sem=x_rcv.at[self.u, k], device_id=dev, device_id_type=MESH)

        def swap(self):
            return self.copy(self.part(1 - me, 0, BLK), d2d.at[self.u], 0, mate, 2)

        def half(self, t):
            n = self.level[t][1]
            return (n // 2, True) if n % 16 == 0 else (n, False)

        def rs(self, t, q):
            _, n, _, fwd, bwd = self.level[t]
            h, _ = self.half(t)
            r1, r2 = rbufs[t]
            src, dst, dev = ((self.spot(t, 2), r1.at[self.u, 0], fwd), (self.spot(t, 2, h), r1.at[self.u, 1], bwd),
                             (self.spot(t, 1), r2.at[self.u, 0], fwd), (self.spot(t, side - 1), r2.at[self.u, 1], bwd))[q]
            return self.copy(self.own(src, h if q < 2 else n), dst, 1 + 4 * t + q, {"tp": dev}, q % 2)

        def ag(self, t, q):
            _, n, _, fwd, bwd = self.level[t]
            h, _ = self.half(t)
            at, m, dev = ((self.spot(t, 0), n, fwd), (self.spot(t, 0), n, bwd),
                          (self.spot(t, side - 1), h, fwd), (self.spot(t, 1, h), h, bwd))[q]
            r = self.out(at, m)
            return self.copy(r, r, 13 + 4 * t + q, {"tp": dev}, q % 2)

        def sent(self, k):
            if k < 1:
                return []
            if k < 7:
                t, second = divmod(k - 1, 2)
                qs, f = ((2, 3) if second else (0, 1) if self.half(t)[1] else (0,)), self.rs
            else:
                t, second = divmod(k - 7, 2)
                t = 2 - t
                qs, f = ((0, 1) if not second else (2, 3) if self.half(t)[1] else (2,)), self.ag
            return [] if t < 0 else [f(t, q) for q in qs]

        def start_rs(self, t):
            self.rs(t, 0).start()
            if self.half(t)[1]:
                self.rs(t, 1).start()

        def start_ag(self, t):
            self.ag(t, 0).start()
            self.ag(t, 1).start()

        def stage(self, k):
            for cpy in self.sent(k - 1):
                cpy.wait_send()
            if k == 1:
                self.swap().wait_recv()
                r = self.own(0, BLK)
                r[...] = r[...] + d2d[self.u]
                self.start_rs(0)
            elif k < 8:
                t, last = divmod(k - 2, 2)
                n = self.level[t][1]
                h, two = self.half(t)
                r1, r2 = rbufs[t]
                if not last:
                    self.rs(t, 0).wait_recv()
                    p = self.own(self.spot(t, 1), h)
                    p[...] = p[...] + r1[self.u, 0]
                    self.rs(t, 2).start()
                    if two:
                        self.rs(t, 1).wait_recv()
                        p = self.own(self.spot(t, side - 1, h), h)
                        p[...] = p[...] + r1[self.u, 1]
                    self.rs(t, 3).start()
                else:
                    self.rs(t, 2).wait_recv()
                    self.rs(t, 3).wait_recv()
                    p = self.own(self.spot(t, 0), n)
                    total = p[...] + r2[self.u, 0] + r2[self.u, 1]
                    if t < 2:
                        p[...] = total
                        self.start_rs(t + 1)
                    else:
                        self.out(self.spot(t, 0), n)[...] = total
                        self.start_ag(2)
            else:
                t, last = divmod(k - 8, 2)
                t = 2 - t
                two = self.half(t)[1]
                if not last:
                    self.ag(t, 0).wait_recv()
                    self.ag(t, 2).start()
                    self.ag(t, 1).wait_recv()
                    if two:
                        self.ag(t, 3).start()
                else:
                    self.ag(t, 2).wait_recv()
                    if two:
                        self.ag(t, 3).wait_recv()
                    if t > 0:
                        self.start_ag(t - 1)

    n_stage = 14

    def each(name, fn):
        for wh, n, turn in sets[name]:
            def body(b, cc, wh=wh, turn=turn):
                fn(Unit(wh, b, turn))
                return cc
            lax.fori_loop(0, n, body, 0)

    def run_stage(k, name):
        each(name, lambda un: un.stage(k))

    def run_for(core, items):
        @pl.when(me == core)
        def _():
            for name, k in items:
                if k == 0:
                    each(name, lambda un: un.swap().start())
                else:
                    run_stage(k, name)

    def hook(t):
        for at in sorted(HOOKS):
            @pl.when(t == at)
            def _(at=at):
                for core in range(2):
                    items = [(name, k) for c, name, k in HOOKS[at] if c == core]
                    if items:
                        run_for(core, items)

    def bwd_core(j, q_rows, kt, mask, first, dq_at):
        q = qt_scr[:, q_rows]
        do = do_scr[q_rows, :]
        s = mm(kc_scr[blk(j), :], q)
        p = jnp.exp2(s * scale2 - lse_scr[:, q_rows])
        if mask is not None:
            p = jnp.where(mask, p, 0.0)
        dp = mm_nt(v_scr[blk(j), :], do)
        ds = (p * (dp - dd_scr[:, q_rows])).astype(BF)
        dq_at[...] += mm(kt, ds)
        dk_blk = mm_nt(ds, q)
        dv_blk = mm(p.astype(BF), do)
        if first:
            dk_scr[...] = dk_blk
            dv_scr[...] = dv_blk
        else:
            dk_scr[...] += dk_blk
            dv_scr[...] += dv_blk

    def bwd_block(step, carry):
        pair, low = step // per, lax.rem(step, per)
        g = jnp.where(pair == 0, 3, jnp.where(pair == 1, 0, jnp.where(pair == 2, 2, 1)))
        j = g * per + 1 - low
        odd = 1 - low
        t0 = jnp.where(pair == 0, low, jnp.where(pair == 1, 2 + 4 * low, jnp.where(pair == 2, 10 + 2 * low, 14 + 3 * low)))
        off = mul(odd * BLK, BLK)

        def body(i, cc):
            hook(t0 + (i - g))

            @pl.when((i == g) & (odd == 1))
            def _():
                high = pl.ds(mul(g * piece + BLK, BLK), BLK)
                bwd_core(j, high, kt_scr[g, :, BLK:], cut(BLK, BLK), True, dqt_scr.at[g, :, BLK:])

            @pl.when((i == g) & (odd == 0))
            def _():
                bwd_core(j, pl.ds(mul(g * piece, piece), piece), kt_scr[g, :, :BLK], cut(BLK, piece), True, dqt_scr.at[g])

            @pl.when(i > g)
            def _():
                bwd_core(j, pl.ds(mul(i * piece, piece), piece), kt_scr[g, :, pl.ds(off, BLK)], None, False, dqt_scr.at[i])

            return cc

        lax.fori_loop(g, 4, body, 0)
        rows = blk(j)
        dk = dk_scr[...] * scale
        dkb = dk[:, :dn].astype(BF)
        dvb = dv_scr[...].astype(BF)
        dkv_scr[rows, :dn] = dkb
        dkv_scr[rows, dn:] = dvb
        dcp[rows, :] = mm_nt(dkv_scr[rows, :], wkv_scr[...])
        drt = dk[:, dn:].T
        owner = jnp.where((g == 0) | (g == 3), 0, 1)
        lt0 = (g // 2) * (piece // LANES) + odd * (BLK // LANES)
        lts = 2 * piece // LANES
        for rt in range(dr // 8):
            b, r = divmod(rt * lts * 8, BLK)
            for lt in range(BLK // LANES):
                row = mul(t_all + owner * BLK + r + (lt0 + lt) * 8, 8)
                dcp[pl.ds(row, 8), b * LANES:(b + 1) * LANES] = drt[rt * 8:rt * 8 + 8, lt * LANES:(lt + 1) * LANES]
        return carry

    def d_weights(lo_j, hi_j):
        def body(j, cc):
            rows = blk(j)
            dw_scr[...] += mm_tn(c_scr[rows, :], dkv_scr[rows, :])
            return cc

        lax.fori_loop(lo_j, hi_j, body, 0)

    def x_o(w):
        g = own_piece(w)
        far_g = (1 - me) if w == 0 else 2 + me
        return pltpu.make_async_remote_copy(src_ref=o_scr.at[pl.ds(mul(far_g * piece, piece), piece), :],
                                            dst_ref=o_far.at[pl.ds(w * piece, piece), :],
                                            send_sem=out_snd.at[w], recv_sem=out_rcv.at[w],
                                            device_id=mate, device_id_type=MESH)

    def x_w():
        return pltpu.make_async_remote_copy(src_ref=dw_scr, dst_ref=dw_far, send_sem=out_snd.at[2], recv_sem=out_rcv.at[2],
                                            device_id=mate, device_id_type=MESH)

    def x_q(w):
        far_g = (1 - me) if w == 0 else 2 + me
        return pltpu.make_async_remote_copy(src_ref=dqt_scr.at[far_g], dst_ref=dqt_out.at[me, :, pl.ds(w * piece, piece)],
                                            send_sem=out_snd.at[4 + w], recv_sem=out_rcv.at[4 + w],
                                            device_id=mate, device_id_type=MESH)

    for w in range(2):
        x_o(w).start()
    for g in range(4):
        dqt_scr[g] = jnp.zeros(dqt_scr.shape[1:], F32)
    dw_scr[...] = jnp.zeros_like(dw_scr)
    lax.fori_loop(0, nb, bwd_block, 0)

    def tail(k):
        for core in range(2):
            items = [(n, k + d) for c, n, d in TAIL if c == core and (k + d > 0) and k + d < n_stage]
            items += [(n, 0) for c, n, d in TAIL if c == 1 - core and k + d == 0]
            if items:
                run_for(core, items)

    tail(0)
    for g in range(4):
        dqt_scr[g] = dqt_scr[g] * scale
    for w in range(2):
        x_q(w).start()
    tail(1)
    d_weights(0, nb // 2)
    tail(2)
    d_weights(nb // 2, nb)
    x_w().start()
    tail(3)
    for w in range(2):
        dqt_out[me, :, pl.ds(w * piece, piece)] = dqt_scr[own_piece(w)]
    tail(4)
    for w in range(2):
        x_o(w).wait_recv()
        mine = o_scr[pl.ds(mul(own_piece(w) * piece, piece), piece), :]
        o_out[pl.ds(w * piece, piece)] = pack(dkv_scr.at[pl.ds(0, piece), :], mine, o_far[pl.ds(w * piece, piece), :])
    tail(5)
    x_w().wait_recv()
    for o_, lo_ in ((dwk_out, 0), (dwv_out, dn)):
        o_[...] = pack(wide_scr, dw_scr[:, lo_:lo_ + dn], dw_far[:, lo_:lo_ + dn])
    for k in range(6, n_stage):
        tail(k)
    for rt in range(dr // 8):
        for lt in range(2 * piece // LANES):
            b, r = divmod((rt * (2 * piece // LANES) + lt) * 8, BLK)
            r += 2 * piece
            drt_out[rt * 8:rt * 8 + 8, lt * LANES:(lt + 1) * LANES] = sum_out[r:r + 8, b * LANES:(b + 1) * LANES]
    for w in range(2):
        x_q(w).wait()
        x_o(w).wait_send()
        for k in range(4):
            in_remote(w, own_piece(w), k).wait_send()

    x_w().wait_send()

    for wh, n in ((0, cols), (1, cols), (2, cols), (3, cols), (4, 2)):
        def drain(b, cc, wh=wh):
            un = Unit(wh, b, 0)
            un.swap().wait_send()
            return cc

        lax.fori_loop(0, n, drain, 0)


def run(c, rt, qt, do, wuk, wuv, side, vmem=51 * 2**20):
    half, rank = c.shape
    t = 2 * half
    dr = rt.shape[0]
    qk = qt.shape[1]
    dn = wuk.shape[2]
    dv = wuv.shape[2]
    nb = t // BLK
    piece = t // 4
    nu = 4 * (rank // LANES) + 2
    sds = jax.ShapeDtypeStruct
    vm = pltpu.VMEM
    bufs = []
    size = BLK
    for _ in range(3):
        n = size // side
        h = n // 2 if n % 16 == 0 else n
        bufs += [vm((nu, 2, h, LANES), F32), vm((nu, 2, n, LANES), F32)]
        size = n
    dma = pltpu.SemaphoreType.DMA
    any_spec = pl.BlockSpec(memory_space=pl.ANY)
    vm_spec = pl.BlockSpec(memory_space=pltpu.VMEM)
    return pl.pallas_call(
        functools.partial(kernel, side),
        in_specs=[any_spec] * 4 + [vm_spec] * 2,
        out_specs=[vm_spec] * 6,
        out_shape=[vm((half, 2, dv), BF), vm((2, qk, half), F32), vm((half + BLK, rank), F32), vm((dr, half), F32),
                   vm((rank, 2, dn), F32), vm((rank, 2, dv), F32)],
        scratch_shapes=[vm((t, rank), BF), vm((dr, t), BF), vm((qk, t), BF), vm((t, 2, dv), BF), vm((rank, dn + dv), BF),
                        vm((t, dv), BF), vm((t, qk), BF), vm((t, dv), BF), vm((4, qk, piece), BF), vm((4, dv, piece), BF),
                        vm((t, dv), BF), vm((1, t), F32), vm((1, t), F32),
                        vm((1, piece), F32), vm((1, piece), F32), vm((dv, piece), F32), vm((4, qk, piece), F32),
                        vm((BLK, qk), F32), vm((BLK, dv), F32), vm((t, dn + dv), BF), vm((rank, 2 * dn), F32),
                        vm((t + 2 * BLK, rank), F32), vm((rank, dn + dv), F32),
                        vm((half, dv), BF), vm((rank, dn + dv), F32), vm((nu, BLK, LANES), F32)]
        + bufs + [dma((4, 2)), dma((4, 2)), dma((4, 2)), dma((nu, 3)), dma((nu, 25)), dma((6,)), dma((6,))],
        compiler_params=pltpu.CompilerParams(collective_id=0, has_side_effects=True, vmem_limit_bytes=vmem),
        name="mla_step",
    )(c, rt, qt, do, wuk, wuv)


def solution(mesh):
    side = round(mesh.shape['tp'] ** (1 / 3))
    seq_spec = P(('dp', 'cp'), None)
    head_spec = P(('dp', 'cp'), 'tp', None)
    weight_spec = P(None, 'tp', None)
    grad_spec = P('dp', 'tp', None)

    def device_fn(c_latent, k_rope, q_heads, d_out, w_uk, w_uv):
        o, dqt, dc, drt, dwk, dwv = run(c_latent, k_rope.T, jnp.transpose(q_heads, (1, 2, 0)), d_out, w_uk, w_uv, side)
        return o, jnp.transpose(dqt, (2, 0, 1)), dc[:c_latent.shape[0]], drt.T, dwk, dwv

    return jax.shard_map(device_fn, mesh=mesh,
                         in_specs=(seq_spec, seq_spec, head_spec, head_spec, weight_spec, weight_spec),
                         out_specs=(head_spec, head_spec, seq_spec, seq_spec, grad_spec, grad_spec),
                         check_vma=False)
```

```python
import functools
import math
import jax
import jax.numpy as jnp
from jax import lax
from jax.experimental import pallas as pl
from jax.experimental.pallas import tpu as pltpu
from jax.sharding import PartitionSpec as P
BF = jnp.bfloat16
F32 = jnp.float32
NEG_BIG = -1.0e30
LOG2E = math.log2(math.e)
LANES = 128
WIDE = 256
BLK = 512
HOOKS = {2: [(1, "p3", 0)], 5: [(0, "p3", 1)], 8: [(0, "p3", 2)], 10: [(1, "p0", 0)], 11: [(0, "p3", 3)],
         13: [(0, "p3", 4), (0, "p0", 1)], 14: [(0, "p2", 0)], 15: [(0, "p3", 5)], 16: [(0, "p0", 2)],
         17: [(0, "p3", 6), (1, "p2", 1), (0, "p1h", 0)], 19: [(0, "p3", 7), (0, "p0", 3), (1, "p2", 2), (1, "p1h", 1)]}
TAIL = ((1, "p1l", 0), (0, "p0", 4), (0, "p3", 8), (1, "p1h", 2), (1, "p2", 3))
MESH = pl.DeviceIdType.MESH


def mm(a, b):
    return lax.dot_general(a, b, (((1,), (0,)), ((), ())), preferred_element_type=F32)


def mm_nt(a, b):
    return lax.dot_general(a, b, (((1,), (1,)), ((), ())), preferred_element_type=F32)


def mm_tn(a, b):
    return lax.dot_general(a, b, (((0,), (0,)), ((), ())), preferred_element_type=F32)


def kernel(side, c_in, rt_in, qt_in, do_in, wuk_in, wuv_in,
           o_out, dqt_out, sum_out, drt_out, dwk_out, dwv_out,
           c_scr, rt_scr, qt_scr, dor_scr, wkv_scr,
           do_scr, kc_scr, v_scr, kt_scr, vt_scr, o_scr, lse_scr, dd_scr,
           m_scr, l_scr, acc_scr, dqt_scr, dk_scr, dv_scr,
           dkv_scr, wide_scr, dcp, dw_scr, o_far, dw_far, d2d,
           ra1, ra2, far1, far2,
           in_loc, in_snd, in_rcv, x_snd, x_rcv, out_snd, out_rcv):
    tp = lax.axis_index("tp")
    me = lax.axis_index("cp")
    strides = (1, side, side * side)
    coord = [lax.rem(tp // st, side) for st in strides]
    nbr = [[tp + (lax.rem(coord[a] + off, side) - coord[a]) * strides[a] for off in range(1, side)] for a in range(3)]
    mate = {"cp": 1 - me}
    t_all, rank = c_scr.shape
    piece = t_all // 4
    nb = t_all // BLK
    per = piece // BLK
    qk = qt_scr.shape[0]
    dn = dwk_out.shape[2]
    dr = rt_scr.shape[0]
    scale = qk ** -0.5
    scale2 = scale * LOG2E
    cols = rank // WIDE

    def mul(x, n):
        return pl.multiple_of(x, n)

    barrier = pltpu.get_barrier_semaphore()
    for a in range(3):
        for b in range(side - 1):
            pl.semaphore_signal(barrier, inc=1, device_id={"tp": nbr[a][b]}, device_id_type=MESH)
    pl.semaphore_signal(barrier, inc=1, device_id=mate, device_id_type=MESH)
    pl.semaphore_wait(barrier, 3 * (side - 1) + 1)

    def own_piece(w):
        return jnp.where(w == 0, me, 3 - me) if not isinstance(w, int) else (me if w == 0 else 3 - me)

    def in_refs(w, g, head):
        src = pl.ds(mul(w * piece, piece), piece)
        dst = pl.ds(mul(g * piece, piece), piece)
        return [(c_in.at[src, :], c_scr.at[dst, :]), (rt_in.at[:, src], rt_scr.at[:, dst]),
                (qt_in.at[head, :, src], qt_scr.at[:, dst]), (do_in.at[src], dor_scr.at[dst])]

    def in_local(w, g, k):
        s, d = in_refs(w, g, me)[k]
        return pltpu.make_async_copy(s, d, in_loc.at[k, w])

    def in_remote(w, g, k):
        s, d = in_refs(w, g, 1 - me)[k]
        return pltpu.make_async_remote_copy(src_ref=s, dst_ref=d, send_sem=in_snd.at[k, w], recv_sem=in_rcv.at[k, w],
                                            device_id=mate, device_id_type=MESH)

    for w in range(2):
        for k in range(4):
            in_local(w, own_piece(w), k).start()
            in_remote(w, own_piece(w), k).start()

    def unpack(x):
        x = x.reshape(x.shape[0], 2 * x.shape[2])
        d = x.shape[1] // 2
        return jnp.where(me == 0, x[:, :d], x[:, d:])

    def pack(buf, mine, other):
        d = mine.shape[1]
        buf[:, :d] = jnp.where(me == 0, mine, other)
        buf[:, d:] = jnp.where(me == 0, other, mine)
        return buf[...].reshape(buf.shape[0], 2, d)

    wkv_scr[:, :dn] = unpack(wuk_in[...])
    wkv_scr[:, dn:] = unpack(wuv_in[...])

    def blk(i):
        return pl.ds(mul(i * BLK, BLK), BLK)

    def lo(n):
        return pl.ds(0, n)

    def soft_update(s, vt, cols, first):
        m_blk = jnp.max(s, axis=0, keepdims=True)
        m_new = m_blk if first else jnp.maximum(m_scr[:, cols], m_blk)
        e = jnp.exp2(s * scale2 - m_new * scale2)
        l_blk = jnp.sum(e, axis=0, keepdims=True)
        o_blk = mm(vt, e.astype(BF))
        if first:
            l_scr[:, cols] = l_blk
            acc_scr[:, cols] = o_blk
        else:
            alpha = jnp.exp2((m_scr[:, cols] - m_new) * scale2)
            l_scr[:, cols] = l_scr[:, cols] * alpha + l_blk
            acc_scr[:, cols] = acc_scr[:, cols] * alpha + o_blk
        m_scr[:, cols] = m_new

    def cut(n_k, n_q):
        kp = lax.broadcasted_iota(jnp.int32, (n_k, n_q), 0)
        qp = lax.broadcasted_iota(jnp.int32, (n_k, n_q), 1)
        return kp <= qp

    def fwd_piece(g, carry):
        w = g // 2
        mine = (g == me) | (g == 3 - me)

        @pl.when(mine)
        def _():
            for k in range(4):
                in_local(w, g, k).wait()

        @pl.when(jnp.logical_not(mine))
        def _():
            for k in range(4):
                in_remote(w, g, k).wait_recv()

        rows = pl.ds(mul(g * piece, piece), piece)
        cb = c_scr[rows, :]
        kv = mm(cb, wkv_scr[...])
        kb, vb = kv[:, :dn], kv[:, dn:]
        rtb = rt_scr[:, rows]
        kc_scr[rows, :dn] = kb.astype(BF)
        kc_scr[rows, dn:] = rtb.astype(F32).T.astype(BF)
        kt_scr[g, :dn, :] = kb.T.astype(BF)
        kt_scr[g, dn:, :] = rtb
        v_scr[rows, :] = vb.astype(BF)
        vt_scr[g] = vb.T.astype(BF)
        do = unpack(dor_scr[rows])
        do_scr[rows, :] = do
        qt = qt_scr[:, rows]
        low = pl.ds(mul(g * piece, piece), BLK)
        high = pl.ds(mul(g * piece + BLK, BLK), BLK)
        s = mm(kc_scr[low, :], qt)
        soft_update(jnp.where(cut(BLK, piece), s, NEG_BIG), vt_scr[g, :, :BLK], slice(None), True)
        s = mm(kc_scr[high, :], qt_scr[:, high])
        soft_update(jnp.where(cut(BLK, BLK), s, NEG_BIG), vt_scr[g, :, BLK:], slice(BLK, piece), False)

        def body(j, cc):
            fwd_full(g, j)
            return cc

        lax.fori_loop(0, g, body, 0)
        ot = acc_scr[...] / l_scr[...]
        o_scr[rows, :] = ot.T.astype(BF)
        dd_scr[:, rows] = jnp.sum(do.astype(F32).T * ot, axis=0, keepdims=True)
        lse_scr[:, rows] = m_scr[...] * scale2 + jnp.log2(l_scr[...])
        return carry

    ra, rb, cs = 128, 256, BLK

    def fwd_full(g, j):
        mx, st = {}, {}
        bufs = (dcp.at[:piece, :], dcp.at[piece:2 * piece, :])

        def score(c, r):
            s = mm(kc_scr[pl.ds(mul(j * piece + r * ra, ra), ra), :], qt_scr[:, pl.ds(mul(g * piece + c * cs, cs), cs)])
            bufs[c % 2][r * ra:(r + 1) * ra, :] = s
            p = jnp.max(s, axis=0, keepdims=True)
            mx[c] = p if c not in mx else jnp.maximum(mx[c], p)

        def mid(c):
            cols = slice(c * cs, (c + 1) * cs)
            m_old = m_scr[:, cols]
            m_new = jnp.maximum(m_old, mx[c])
            m_scr[:, cols] = m_new
            st[c] = [m_new * scale2, jnp.exp2((m_old - m_new) * scale2), None, None]

        def weigh(c, r):
            d = st[c]
            e = jnp.exp2(bufs[c % 2][r * rb:(r + 1) * rb, :] * scale2 - d[0])
            p = jnp.sum(e, axis=0, keepdims=True)
            o = mm(vt_scr[j, :, r * rb:(r + 1) * rb], e.astype(BF))
            d[2] = p if d[2] is None else d[2] + p
            d[3] = o if d[3] is None else d[3] + o

        def fin(c):
            cols = slice(c * cs, (c + 1) * cs)
            d = st[c]
            l_scr[:, cols] = l_scr[:, cols] * d[1] + d[2]
            acc_scr[:, cols] = acc_scr[:, cols] * d[1] + d[3]

        na, nr = piece // ra, piece // rb
        for r in range(na):
            score(0, r)
        for c in range(piece // cs):
            mid(c)
            for r in range(na):
                if c + 1 < piece // cs:
                    score(c + 1, r)
                if r % (na // nr) == na // nr - 1:
                    weigh(c, r // (na // nr))
            fin(c)

    lax.fori_loop(0, 4, fwd_piece, 0)

    sets = {"p3": ((2, cols, 0), (3, cols, 2)), "p0": ((0, cols, 1), (1, cols, 0), (4, 1, 2)),
            "p2": ((2, cols, 0), (3, cols, 2)), "p1h": ((1, cols, 1),), "p1l": ((0, cols, 0), (4, 1, 2))}

    def pick(a, xs):
        return jnp.where(a == 0, xs[0], jnp.where(a == 1, xs[1], xs[2]))

    def wrap(x, n):
        return jnp.where(x >= n, x - n, x)

    class Unit:
        def __init__(self, wh, b, turn):
            self.wh = wh
            self.u = wh * cols + b
            self.lanes = pl.ds(mul(b * WIDE, WIDE), WIDE)
            first = wrap(b + turn, 3)
            self.level = []
            base, size = 0, BLK
            for t in range(3):
                a = wrap(first + t, 3)
                n = size // side
                here = pick(a, coord)
                self.level.append((base, n, here, [pick(a, [x[o] for x in nbr]) for o in range(side - 1)]))
                base, size = base + here * n, n

        def part(self, owner, start, n):
            if self.wh == 4:
                top = t_all + owner * BLK
            else:
                top = (owner if self.wh < 2 else 3 - owner) * piece + (self.wh % 2) * BLK
            return dcp.at[pl.ds(mul(top + start, 8), n), self.lanes]

        def own(self, start, n):
            return self.part(me, start, n)

        def out(self, start, n):
            return sum_out.at[pl.ds(mul(self.wh * BLK + start, 8), n), self.lanes]

        def spot(self, t, off, extra=0):
            base, n, here, _ = self.level[t]
            return base + wrap(here + off, side) * n + extra

        def copy(self, src, dst, k, dev, slot):
            return pltpu.make_async_remote_copy(src_ref=src, dst_ref=dst, send_sem=x_snd.at[self.u, slot],
                                                recv_sem=x_rcv.at[self.u, k], device_id=dev, device_id_type=MESH)

        def swap(self):
            return self.copy(self.part(1 - me, 0, BLK), d2d.at[self.u], 0, mate, 3)

        def near(self, q):
            _, n, _, dev = self.level[0]
            h = n // 2
            src, m, dst, to = ((self.spot(0, 2), h, ra1.at[self.u, 0], 0), (self.spot(0, 2, h), h, ra1.at[self.u, 1], 2),
                               (self.spot(0, 1), n, ra2.at[self.u, 0], 0), (self.spot(0, side - 1), n, ra2.at[self.u, 1], 2))[q]
            return self.copy(self.own(src, m), dst, 1 + q, {"tp": dev[to]}, q % 2)

        def back(self, q):
            _, n, _, dev = self.level[0]
            h = n // 2
            at, m, to = ((self.spot(0, 0), n, 0), (self.spot(0, 0), n, 2),
                         (self.spot(0, side - 1), h, 0), (self.spot(0, 1, h), h, 2))[q]
            r = self.out(at, m)
            return self.copy(r, r, 5 + q, {"tp": dev[to]}, q % 2)

        def direct(self, t, o):
            _, n, _, dev = self.level[t]
            return self.copy(self.own(self.spot(t, o + 1), n), (far1, far2)[t - 1].at[self.u, o], 9 + 3 * (t - 1) + o,
                             {"tp": dev[o]}, o)

        def share(self, t, o):
            _, n, _, dev = self.level[t]
            r = self.out(self.spot(t, 0), n)
            return self.copy(r, r, 15 + 3 * (t - 1) + o, {"tp": dev[o]}, o)

        def started(self, k):
            return {1: lambda: [self.near(0), self.near(1)], 2: lambda: [self.near(2), self.near(3)],
                    3: lambda: [self.direct(1, o) for o in range(3)], 4: lambda: [self.direct(2, o) for o in range(3)],
                    5: lambda: [self.share(2, o) for o in range(3)], 6: lambda: [self.share(1, o) for o in range(3)],
                    7: lambda: [self.back(0), self.back(1)], 8: lambda: [self.back(2), self.back(3)]}.get(k, lambda: [])()

        def stage(self, k):
            for cpy in self.started(k - 1):
                cpy.wait_send()
            u = self.u
            if k == 1:
                self.swap().wait_recv()
                r = self.own(0, BLK)
                r[...] = r[...] + d2d[u]
            elif k == 2:
                h = self.level[0][1] // 2
                for q, at in ((0, self.spot(0, 1)), (1, self.spot(0, side - 1, h))):
                    self.near(q).wait_recv()
                    p = self.own(at, h)
                    p[...] = p[...] + ra1[u, q]
            elif k in (3, 4, 5):
                t = k - 3
                for cpy in ([self.near(2), self.near(3)] if t == 0 else [self.direct(t, o) for o in range(3)]):
                    cpy.wait_recv()
                at, n = self.spot(t, 0), self.level[t][1]
                total = self.own(at, n)[...]
                for o in range(2 if t == 0 else 3):
                    total = total + (ra2, far1, far2)[t][u, o]
                (self.out if t == 2 else self.own)(at, n)[...] = total
            elif k > 5:
                for cpy in self.started(k - 1):
                    cpy.wait_recv()
            for cpy in self.started(k):
                cpy.start()

    n_stage = 10

    def each(name, fn):
        for wh, n, turn in sets[name]:
            def body(b, cc, wh=wh, turn=turn):
                fn(Unit(wh, b, turn))
                return cc
            lax.fori_loop(0, n, body, 0)

    def run_stage(k, name):
        each(name, lambda un: un.stage(k))

    def run_for(core, items):
        @pl.when(me == core)
        def _():
            for name, k in items:
                if k == 0:
                    each(name, lambda un: un.swap().start())
                else:
                    run_stage(k, name)

    def hook(t):
        for at in sorted(HOOKS):
            @pl.when(t == at)
            def _(at=at):
                for core in range(2):
                    items = [(name, k) for c, name, k in HOOKS[at] if c == core]
                    if items:
                        run_for(core, items)

    def bwd_core(j, q_rows, kt, mask, first, dq_at):
        q = qt_scr[:, q_rows]
        do = do_scr[q_rows, :]
        s = mm(kc_scr[blk(j), :], q)
        p = jnp.exp2(s * scale2 - lse_scr[:, q_rows])
        if mask is not None:
            p = jnp.where(mask, p, 0.0)
        dp = mm_nt(v_scr[blk(j), :], do)
        ds = (p * (dp - dd_scr[:, q_rows])).astype(BF)
        dq_at[...] += mm(kt, ds)
        dk_blk = mm_nt(ds, q)
        dv_blk = mm(p.astype(BF), do)
        if first:
            dk_scr[...] = dk_blk
            dv_scr[...] = dv_blk
        else:
            dk_scr[...] += dk_blk
            dv_scr[...] += dv_blk

    def bwd_block(step, carry):
        pair, low = step // per, lax.rem(step, per)
        g = jnp.where(pair == 0, 3, jnp.where(pair == 1, 0, jnp.where(pair == 2, 2, 1)))
        j = g * per + 1 - low
        odd = 1 - low
        t0 = jnp.where(pair == 0, low, jnp.where(pair == 1, 2 + 4 * low, jnp.where(pair == 2, 10 + 2 * low, 14 + 3 * low)))
        off = mul(odd * BLK, BLK)

        def body(i, cc):
            hook(t0 + (i - g))

            @pl.when((i == g) & (odd == 1))
            def _():
                high = pl.ds(mul(g * piece + BLK, BLK), BLK)
                bwd_core(j, high, kt_scr[g, :, BLK:], cut(BLK, BLK), True, dqt_scr.at[g, :, BLK:])

            @pl.when((i == g) & (odd == 0))
            def _():
                bwd_core(j, pl.ds(mul(g * piece, piece), piece), kt_scr[g, :, :BLK], cut(BLK, piece), True, dqt_scr.at[g])

            @pl.when(i > g)
            def _():
                bwd_core(j, pl.ds(mul(i * piece, piece), piece), kt_scr[g, :, pl.ds(off, BLK)], None, False, dqt_scr.at[i])

            return cc

        lax.fori_loop(g, 4, body, 0)
        rows = blk(j)
        dk = dk_scr[...] * scale
        dkb = dk[:, :dn].astype(BF)
        dvb = dv_scr[...].astype(BF)
        dkv_scr[rows, :dn] = dkb
        dkv_scr[rows, dn:] = dvb
        dcp[rows, :] = mm_nt(dkv_scr[rows, :], wkv_scr[...])
        drt = dk[:, dn:].T
        owner = jnp.where((g == 0) | (g == 3), 0, 1)
        lt0 = (g // 2) * (piece // LANES) + odd * (BLK // LANES)
        lts = 2 * piece // LANES
        for rt in range(dr // 8):
            b, r = divmod(rt * lts * 8, BLK)
            for lt in range(BLK // LANES):
                row = mul(t_all + owner * BLK + r + (lt0 + lt) * 8, 8)
                dcp[pl.ds(row, 8), b * LANES:(b + 1) * LANES] = drt[rt * 8:rt * 8 + 8, lt * LANES:(lt + 1) * LANES]
        return carry

    def d_weights(lo_j, hi_j):
        def body(j, cc):
            rows = blk(j)
            dw_scr[...] += mm_tn(c_scr[rows, :], dkv_scr[rows, :])
            return cc

        lax.fori_loop(lo_j, hi_j, body, 0)

    def x_o(w):
        g = own_piece(w)
        far_g = (1 - me) if w == 0 else 2 + me
        return pltpu.make_async_remote_copy(src_ref=o_scr.at[pl.ds(mul(far_g * piece, piece), piece), :],
                                            dst_ref=o_far.at[pl.ds(w * piece, piece), :],
                                            send_sem=out_snd.at[w], recv_sem=out_rcv.at[w],
                                            device_id=mate, device_id_type=MESH)

    def x_w():
        return pltpu.make_async_remote_copy(src_ref=dw_scr, dst_ref=dw_far, send_sem=out_snd.at[2], recv_sem=out_rcv.at[2],
                                            device_id=mate, device_id_type=MESH)

    def x_q(w):
        far_g = (1 - me) if w == 0 else 2 + me
        return pltpu.make_async_remote_copy(src_ref=dqt_scr.at[far_g], dst_ref=dqt_out.at[me, :, pl.ds(w * piece, piece)],
                                            send_sem=out_snd.at[4 + w], recv_sem=out_rcv.at[4 + w],
                                            device_id=mate, device_id_type=MESH)

    for w in range(2):
        x_o(w).start()
    for g in range(4):
        dqt_scr[g] = jnp.zeros(dqt_scr.shape[1:], F32)
    dw_scr[...] = jnp.zeros_like(dw_scr)
    lax.fori_loop(0, nb, bwd_block, 0)

    def tail(k):
        for core in range(2):
            items = [(n, k + d) for c, n, d in TAIL if c == core and (k + d > 0) and k + d < n_stage]
            items += [(n, 0) for c, n, d in TAIL if c == 1 - core and k + d == 0]
            if items:
                run_for(core, items)

    tail(0)
    for g in range(4):
        dqt_scr[g] = dqt_scr[g] * scale
    for w in range(2):
        x_q(w).start()
    tail(1)
    d_weights(0, nb // 2)
    tail(2)
    d_weights(nb // 2, nb)
    x_w().start()
    tail(3)
    for w in range(2):
        dqt_out[me, :, pl.ds(w * piece, piece)] = dqt_scr[own_piece(w)]
    tail(4)
    for w in range(2):
        x_o(w).wait_recv()
        mine = o_scr[pl.ds(mul(own_piece(w) * piece, piece), piece), :]
        o_out[pl.ds(w * piece, piece)] = pack(dkv_scr.at[pl.ds(0, piece), :], mine, o_far[pl.ds(w * piece, piece), :])
    tail(5)
    x_w().wait_recv()
    for o_, lo_ in ((dwk_out, 0), (dwv_out, dn)):
        o_[...] = pack(wide_scr, dw_scr[:, lo_:lo_ + dn], dw_far[:, lo_:lo_ + dn])
    for k in range(6, n_stage):
        tail(k)
    for rt in range(dr // 8):
        for lt in range(2 * piece // LANES):
            b, r = divmod((rt * (2 * piece // LANES) + lt) * 8, BLK)
            r += 2 * piece
            drt_out[rt * 8:rt * 8 + 8, lt * LANES:(lt + 1) * LANES] = sum_out[r:r + 8, b * LANES:(b + 1) * LANES]
    for w in range(2):
        x_q(w).wait()
        x_o(w).wait_send()
        for k in range(4):
            in_remote(w, own_piece(w), k).wait_send()

    x_w().wait_send()

    for wh, n in ((0, cols), (1, cols), (2, cols), (3, cols), (4, 1)):
        def drain(b, cc, wh=wh):
            un = Unit(wh, b, 0)
            un.swap().wait_send()
            return cc

        lax.fori_loop(0, n, drain, 0)


def run(c, rt, qt, do, wuk, wuv, side, vmem=51 * 2**20):
    half, rank = c.shape
    t = 2 * half
    dr = rt.shape[0]
    qk = qt.shape[1]
    dn = wuk.shape[2]
    dv = wuv.shape[2]
    nb = t // BLK
    piece = t // 4
    nu = 4 * (rank // WIDE) + 1
    sds = jax.ShapeDtypeStruct
    vm = pltpu.VMEM
    bufs = []
    size = BLK
    for _ in range(3):
        n = size // side
        h = n // 2 if n % 16 == 0 else n
        bufs += [vm((nu, 2, h, WIDE), F32)] if not bufs else []
        bufs += [vm((nu, 2 if size == BLK else 3, n, WIDE), F32)]
        size = n
    dma = pltpu.SemaphoreType.DMA
    any_spec = pl.BlockSpec(memory_space=pl.ANY)
    vm_spec = pl.BlockSpec(memory_space=pltpu.VMEM)
    return pl.pallas_call(
        functools.partial(kernel, side),
        in_specs=[any_spec] * 4 + [vm_spec] * 2,
        out_specs=[vm_spec] * 6,
        out_shape=[vm((half, 2, dv), BF), vm((2, qk, half), F32), vm((half + BLK, rank), F32), vm((dr, half), F32),
                   vm((rank, 2, dn), F32), vm((rank, 2, dv), F32)],
        scratch_shapes=[vm((t, rank), BF), vm((dr, t), BF), vm((qk, t), BF), vm((t, 2, dv), BF), vm((rank, dn + dv), BF),
                        vm((t, dv), BF), vm((t, qk), BF), vm((t, dv), BF), vm((4, qk, piece), BF), vm((4, dv, piece), BF),
                        vm((t, dv), BF), vm((1, t), F32), vm((1, t), F32),
                        vm((1, piece), F32), vm((1, piece), F32), vm((dv, piece), F32), vm((4, qk, piece), F32),
                        vm((BLK, qk), F32), vm((BLK, dv), F32), vm((t, dn + dv), BF), vm((rank, 2 * dn), F32),
                        vm((t + 2 * BLK, rank), F32), vm((rank, dn + dv), F32),
                        vm((half, dv), BF), vm((rank, dn + dv), F32), vm((nu, BLK, WIDE), F32)]
        + bufs + [dma((4, 2)), dma((4, 2)), dma((4, 2)), dma((nu, 4)), dma((nu, 21)), dma((6,)), dma((6,))],
        compiler_params=pltpu.CompilerParams(collective_id=0, has_side_effects=True, vmem_limit_bytes=vmem),
        name="mla_step",
    )(c, rt, qt, do, wuk, wuv)


def store_kernel(*refs):
    n = (len(refs) - 1) // 2
    sem = refs[-1]
    copies = []
    for k in range(n):
        src, dst = refs[k], refs[n + k]
        if src.shape != dst.shape:
            src = src.at[pl.ds(0, dst.shape[0]), :]
        copies.append(pltpu.make_async_copy(src, dst, sem.at[k]))
    for cpy in copies:
        cpy.start()
    for cpy in copies:
        cpy.wait()


def store_all(arrays, shapes):
    n = len(arrays)
    return pl.pallas_call(
        store_kernel,
        in_specs=[pl.BlockSpec(memory_space=pltpu.VMEM)] * n,
        out_specs=[pl.BlockSpec(memory_space=pl.ANY)] * n,
        out_shape=[pltpu.HBM(sh, a.dtype) for a, sh in zip(arrays, shapes)],
        scratch_shapes=[pltpu.SemaphoreType.DMA((n,))],
        compiler_params=pltpu.CompilerParams(vmem_limit_bytes=2**20),
        name="store_all",
    )(*arrays)


def solution(mesh):
    side = round(mesh.shape['tp'] ** (1 / 3))
    seq_spec = P(('dp', 'cp'), None)
    head_spec = P(('dp', 'cp'), 'tp', None)
    weight_spec = P(None, 'tp', None)
    grad_spec = P('dp', 'tp', None)

    def device_fn(c_latent, k_rope, q_heads, d_out, w_uk, w_uv):
        outs = run(c_latent, k_rope.T, jnp.transpose(q_heads, (1, 2, 0)), d_out, w_uk, w_uv, side)
        shapes = [c_latent.shape if k == 2 else x.shape for k, x in enumerate(outs)]
        o, dqt, dc, drt, dwk, dwv = store_all(outs, shapes)
        return o, jnp.transpose(dqt, (2, 0, 1)), dc, drt.T, dwk, dwv

    return jax.shard_map(device_fn, mesh=mesh,
                         in_specs=(seq_spec, seq_spec, head_spec, head_spec, weight_spec, weight_spec),
                         out_specs=(head_spec, head_spec, seq_spec, seq_spec, grad_spec, grad_spec),
                         check_vma=False)
```

```python
import functools
import math
import jax
import jax.numpy as jnp
from jax import lax
from jax.experimental import pallas as pl
from jax.experimental.pallas import tpu as pltpu
from jax.sharding import PartitionSpec as P
BF = jnp.bfloat16
F32 = jnp.float32
NEG_BIG = -1.0e30
LOG2E = math.log2(math.e)
LANES = 128
WIDE = 256
BLK = 512
ORDER = (7, 6, 1, 5, 4, 0, 3, 2)
SLOTS = (0, 1, 2, 6, 8, 10, 14, 17)
HOOKS = {2: [(1, "p3", 0)], 5: [(0, "p3", 1)], 8: [(0, "p3", 2)], 10: [(0, "p2", 0)], 11: [(0, "p3", 3)],
         13: [(0, "p3", 4), (1, "p2", 1)], 14: [(1, "p0", 0)], 15: [(0, "p3", 5), (1, "p2", 2)], 16: [(0, "p0", 1)],
         17: [(0, "p3", 6), (0, "p1h", 0), (1, "p2", 3)], 19: [(0, "p3", 7), (0, "p0", 2), (1, "p1h", 1)]}
TAIL = ((1, "p1l", 0), (0, "p0", 3), (0, "p3", 8), (1, "p1h", 2), (1, "p2", 4))
MESH = pl.DeviceIdType.MESH


def mm(a, b):
    return lax.dot_general(a, b, (((1,), (0,)), ((), ())), preferred_element_type=F32)


def mm_nt(a, b):
    return lax.dot_general(a, b, (((1,), (1,)), ((), ())), preferred_element_type=F32)


def mm_tn(a, b):
    return lax.dot_general(a, b, (((0,), (0,)), ((), ())), preferred_element_type=F32)


def kernel(side, c_in, rt_in, qt_in, do_in, wuk_in, wuv_in,
           o_out, dqt_out, sum_out, drt_out, dwk_out, dwv_out,
           c_scr, rt_scr, qt_scr, dor_scr, wkv_scr,
           do_scr, kc_scr, v_scr, kt_scr, vt_scr, o_scr, lse_scr, dd_scr,
           m_scr, l_scr, acc_scr, dqt_scr, dk_scr, dv_scr,
           dkv_scr, wide_scr, dcp, dw_scr, o_far, dw_far, d2d,
           ra1, ra2, far1, far2,
           in_loc, in_snd, in_rcv, x_snd, x_rcv, out_snd, out_rcv):
    tp = lax.axis_index("tp")
    me = lax.axis_index("cp")
    strides = (1, side, side * side)
    coord = [lax.rem(tp // st, side) for st in strides]
    nbr = [[tp + (lax.rem(coord[a] + off, side) - coord[a]) * strides[a] for off in range(1, side)] for a in range(3)]
    mate = {"cp": 1 - me}
    t_all, rank = c_scr.shape
    piece = t_all // 4
    nb = t_all // BLK
    per = piece // BLK
    qk = qt_scr.shape[0]
    dn = dwk_out.shape[2]
    dr = rt_scr.shape[0]
    scale = qk ** -0.5
    scale2 = scale * LOG2E
    cols = rank // WIDE

    def mul(x, n):
        return pl.multiple_of(x, n)

    barrier = pltpu.get_barrier_semaphore()
    for a in range(3):
        for b in range(side - 1):
            pl.semaphore_signal(barrier, inc=1, device_id={"tp": nbr[a][b]}, device_id_type=MESH)
    pl.semaphore_signal(barrier, inc=1, device_id=mate, device_id_type=MESH)
    pl.semaphore_wait(barrier, 3 * (side - 1) + 1)

    def own_piece(w):
        return jnp.where(w == 0, me, 3 - me) if not isinstance(w, int) else (me if w == 0 else 3 - me)

    def in_refs(w, g, head):
        src = pl.ds(mul(w * piece, piece), piece)
        dst = pl.ds(mul(g * piece, piece), piece)
        return [(c_in.at[src, :], c_scr.at[dst, :]), (rt_in.at[:, src], rt_scr.at[:, dst]),
                (qt_in.at[head, :, src], qt_scr.at[:, dst]), (do_in.at[src], dor_scr.at[dst])]

    def in_local(w, g, k):
        s, d = in_refs(w, g, me)[k]
        return pltpu.make_async_copy(s, d, in_loc.at[k, w])

    def in_remote(w, g, k):
        s, d = in_refs(w, g, 1 - me)[k]
        return pltpu.make_async_remote_copy(src_ref=s, dst_ref=d, send_sem=in_snd.at[k, w], recv_sem=in_rcv.at[k, w],
                                            device_id=mate, device_id_type=MESH)

    for w in range(2):
        for k in range(4):
            in_local(w, own_piece(w), k).start()
            in_remote(w, own_piece(w), k).start()

    def unpack(x):
        x = x.reshape(x.shape[0], 2 * x.shape[2])
        d = x.shape[1] // 2
        return jnp.where(me == 0, x[:, :d], x[:, d:])

    def pack(buf, mine, other):
        d = mine.shape[1]
        buf[:, :d] = jnp.where(me == 0, mine, other)
        buf[:, d:] = jnp.where(me == 0, other, mine)
        return buf[...].reshape(buf.shape[0], 2, d)

    wkv_scr[:, :dn] = unpack(wuk_in[...])
    wkv_scr[:, dn:] = unpack(wuv_in[...])

    def blk(i):
        return pl.ds(mul(i * BLK, BLK), BLK)

    def lo(n):
        return pl.ds(0, n)

    def soft_update(s, vt, cols, first):
        m_blk = jnp.max(s, axis=0, keepdims=True)
        m_new = m_blk if first else jnp.maximum(m_scr[:, cols], m_blk)
        e = jnp.exp2(s * scale2 - m_new * scale2)
        l_blk = jnp.sum(e, axis=0, keepdims=True)
        o_blk = mm(vt, e.astype(BF))
        if first:
            l_scr[:, cols] = l_blk
            acc_scr[:, cols] = o_blk
        else:
            alpha = jnp.exp2((m_scr[:, cols] - m_new) * scale2)
            l_scr[:, cols] = l_scr[:, cols] * alpha + l_blk
            acc_scr[:, cols] = acc_scr[:, cols] * alpha + o_blk
        m_scr[:, cols] = m_new

    def cut(n_k, n_q):
        kp = lax.broadcasted_iota(jnp.int32, (n_k, n_q), 0)
        qp = lax.broadcasted_iota(jnp.int32, (n_k, n_q), 1)
        return kp <= qp

    def fwd_piece(g, carry):
        w = g // 2
        mine = (g == me) | (g == 3 - me)

        @pl.when(mine)
        def _():
            for k in range(4):
                in_local(w, g, k).wait()

        @pl.when(jnp.logical_not(mine))
        def _():
            for k in range(4):
                in_remote(w, g, k).wait_recv()

        rows = pl.ds(mul(g * piece, piece), piece)
        cb = c_scr[rows, :]
        kv = mm(cb, wkv_scr[...])
        kb, vb = kv[:, :dn], kv[:, dn:]
        rtb = rt_scr[:, rows]
        kc_scr[rows, :dn] = kb.astype(BF)
        kc_scr[rows, dn:] = rtb.astype(F32).T.astype(BF)
        kt_scr[g, :dn, :] = kb.T.astype(BF)
        kt_scr[g, dn:, :] = rtb
        v_scr[rows, :] = vb.astype(BF)
        vt_scr[g] = vb.T.astype(BF)
        do = unpack(dor_scr[rows])
        do_scr[rows, :] = do
        qt = qt_scr[:, rows]
        low = pl.ds(mul(g * piece, piece), BLK)
        high = pl.ds(mul(g * piece + BLK, BLK), BLK)
        s = mm(kc_scr[low, :], qt)
        soft_update(jnp.where(cut(BLK, piece), s, NEG_BIG), vt_scr[g, :, :BLK], slice(None), True)
        s = mm(kc_scr[high, :], qt_scr[:, high])
        soft_update(jnp.where(cut(BLK, BLK), s, NEG_BIG), vt_scr[g, :, BLK:], slice(BLK, piece), False)

        def body(j, cc):
            fwd_full(g, j)
            return cc

        lax.fori_loop(0, g, body, 0)
        ot = acc_scr[...] / l_scr[...]
        o_scr[rows, :] = ot.T.astype(BF)
        dd_scr[:, rows] = jnp.sum(do.astype(F32).T * ot, axis=0, keepdims=True)
        lse_scr[:, rows] = m_scr[...] * scale2 + jnp.log2(l_scr[...])
        return carry

    ra, rb, cs = 128, 256, BLK

    def fwd_full(g, j):
        mx, st = {}, {}
        bufs = (dcp.at[:piece, :], dcp.at[piece:2 * piece, :])

        def score(c, r):
            s = mm(kc_scr[pl.ds(mul(j * piece + r * ra, ra), ra), :], qt_scr[:, pl.ds(mul(g * piece + c * cs, cs), cs)])
            bufs[c % 2][r * ra:(r + 1) * ra, :] = s
            p = jnp.max(s, axis=0, keepdims=True)
            mx[c] = p if c not in mx else jnp.maximum(mx[c], p)

        def mid(c):
            cols = slice(c * cs, (c + 1) * cs)
            m_old = m_scr[:, cols]
            m_new = jnp.maximum(m_old, mx[c])
            m_scr[:, cols] = m_new
            st[c] = [m_new * scale2, jnp.exp2((m_old - m_new) * scale2), None, None]

        def weigh(c, r):
            d = st[c]
            e = jnp.exp2(bufs[c % 2][r * rb:(r + 1) * rb, :] * scale2 - d[0])
            p = jnp.sum(e, axis=0, keepdims=True)
            o = mm(vt_scr[j, :, r * rb:(r + 1) * rb], e.astype(BF))
            d[2] = p if d[2] is None else d[2] + p
            d[3] = o if d[3] is None else d[3] + o

        def fin(c):
            cols = slice(c * cs, (c + 1) * cs)
            d = st[c]
            l_scr[:, cols] = l_scr[:, cols] * d[1] + d[2]
            acc_scr[:, cols] = acc_scr[:, cols] * d[1] + d[3]

        na, nr = piece // ra, piece // rb
        for r in range(na):
            score(0, r)
        for c in range(piece // cs):
            mid(c)
            for r in range(na):
                if c + 1 < piece // cs:
                    score(c + 1, r)
                if r % (na // nr) == na // nr - 1:
                    weigh(c, r // (na // nr))
            fin(c)

    lax.fori_loop(0, 4, fwd_piece, 0)

    sets = {"p3": ((2, cols, 0), (3, cols, 2)), "p0": ((0, cols, 1), (1, cols, 0), (4, 1, 2)),
            "p2": ((2, cols, 0), (3, cols, 2)), "p1h": ((1, cols, 1),), "p1l": ((0, cols, 0), (4, 1, 2))}

    def pick(a, xs):
        return jnp.where(a == 0, xs[0], jnp.where(a == 1, xs[1], xs[2]))

    def wrap(x, n):
        return jnp.where(x >= n, x - n, x)

    class Unit:
        def __init__(self, wh, b, turn):
            self.wh = wh
            self.u = wh * cols + b
            self.lanes = pl.ds(mul(b * WIDE, WIDE), WIDE)
            first = wrap(b + turn, 3)
            self.level = []
            base, size = 0, BLK
            for t in range(3):
                a = wrap(first + t, 3)
                n = size // side
                here = pick(a, coord)
                self.level.append((base, n, here, [pick(a, [x[o] for x in nbr]) for o in range(side - 1)]))
                base, size = base + here * n, n

        def part(self, owner, start, n):
            if self.wh == 4:
                top = t_all + owner * BLK
            else:
                top = (owner if self.wh < 2 else 3 - owner) * piece + (self.wh % 2) * BLK
            return dcp.at[pl.ds(mul(top + start, 8), n), self.lanes]

        def own(self, start, n):
            return self.part(me, start, n)

        def out(self, start, n):
            return sum_out.at[pl.ds(mul(self.wh * BLK + start, 8), n), self.lanes]

        def spot(self, t, off, extra=0):
            base, n, here, _ = self.level[t]
            return base + wrap(here + off, side) * n + extra

        def copy(self, src, dst, k, dev, slot):
            return pltpu.make_async_remote_copy(src_ref=src, dst_ref=dst, send_sem=x_snd.at[self.u, slot],
                                                recv_sem=x_rcv.at[self.u, k], device_id=dev, device_id_type=MESH)

        def swap(self):
            return self.copy(self.part(1 - me, 0, BLK), d2d.at[self.u], 0, mate, 3)

        def near(self, q):
            _, n, _, dev = self.level[0]
            h = n // 2
            src, m, dst, to = ((self.spot(0, 2), h, ra1.at[self.u, 0], 0), (self.spot(0, 2, h), h, ra1.at[self.u, 1], 2),
                               (self.spot(0, 1), n, ra2.at[self.u, 0], 0), (self.spot(0, side - 1), n, ra2.at[self.u, 1], 2))[q]
            return self.copy(self.own(src, m), dst, 1 + q, {"tp": dev[to]}, q % 2)

        def back(self, q):
            _, n, _, dev = self.level[0]
            h = n // 2
            at, m, to = ((self.spot(0, 0), n, 0), (self.spot(0, 0), n, 2),
                         (self.spot(0, side - 1), h, 0), (self.spot(0, 1, h), h, 2))[q]
            r = self.out(at, m)
            return self.copy(r, r, 5 + q, {"tp": dev[to]}, q % 2)

        def direct(self, t, o):
            _, n, _, dev = self.level[t]
            return self.copy(self.own(self.spot(t, o + 1), n), (far1, far2)[t - 1].at[self.u, o], 9 + 3 * (t - 1) + o,
                             {"tp": dev[o]}, o)

        def share(self, t, o):
            _, n, _, dev = self.level[t]
            r = self.out(self.spot(t, 0), n)
            return self.copy(r, r, 15 + 3 * (t - 1) + o, {"tp": dev[o]}, o)

        def started(self, k):
            return {1: lambda: [self.near(0), self.near(1)], 2: lambda: [self.near(2), self.near(3)],
                    3: lambda: [self.direct(1, o) for o in range(3)], 4: lambda: [self.direct(2, o) for o in range(3)],
                    5: lambda: [self.share(2, o) for o in range(3)], 6: lambda: [self.share(1, o) for o in range(3)],
                    7: lambda: [self.back(0), self.back(1)], 8: lambda: [self.back(2), self.back(3)]}.get(k, lambda: [])()

        def stage(self, k):
            for cpy in self.started(k - 1):
                cpy.wait_send()
            u = self.u
            if k == 1:
                self.swap().wait_recv()
                r = self.own(0, BLK)
                r[...] = r[...] + d2d[u]
            elif k == 2:
                h = self.level[0][1] // 2
                for q, at in ((0, self.spot(0, 1)), (1, self.spot(0, side - 1, h))):
                    self.near(q).wait_recv()
                    p = self.own(at, h)
                    p[...] = p[...] + ra1[u, q]
            elif k in (3, 4, 5):
                t = k - 3
                for cpy in ([self.near(2), self.near(3)] if t == 0 else [self.direct(t, o) for o in range(3)]):
                    cpy.wait_recv()
                at, n = self.spot(t, 0), self.level[t][1]
                total = self.own(at, n)[...]
                for o in range(2 if t == 0 else 3):
                    total = total + (ra2, far1, far2)[t][u, o]
                (self.out if t == 2 else self.own)(at, n)[...] = total
            elif k > 5:
                for cpy in self.started(k - 1):
                    cpy.wait_recv()
            for cpy in self.started(k):
                cpy.start()

    n_stage = 10

    def each(name, fn):
        for wh, n, turn in sets[name]:
            def body(b, cc, wh=wh, turn=turn):
                fn(Unit(wh, b, turn))
                return cc
            lax.fori_loop(0, n, body, 0)

    def run_stage(k, name):
        each(name, lambda un: un.stage(k))

    def run_for(core, items):
        @pl.when(me == core)
        def _():
            for name, k in items:
                if k == 0:
                    each(name, lambda un: un.swap().start())
                else:
                    run_stage(k, name)

    def hook(t):
        for at in sorted(HOOKS):
            @pl.when(t == at)
            def _(at=at):
                for core in range(2):
                    items = [(name, k) for c, name, k in HOOKS[at] if c == core]
                    if items:
                        run_for(core, items)

    def bwd_core(j, q_rows, kt, mask, first, dq_at):
        q = qt_scr[:, q_rows]
        do = do_scr[q_rows, :]
        s = mm(kc_scr[blk(j), :], q)
        p = jnp.exp2(s * scale2 - lse_scr[:, q_rows])
        if mask is not None:
            p = jnp.where(mask, p, 0.0)
        dp = mm_nt(v_scr[blk(j), :], do)
        ds = (p * (dp - dd_scr[:, q_rows])).astype(BF)
        dq_at[...] += mm(kt, ds)
        dk_blk = mm_nt(ds, q)
        dv_blk = mm(p.astype(BF), do)
        if first:
            dk_scr[...] = dk_blk
            dv_scr[...] = dv_blk
        else:
            dk_scr[...] += dk_blk
            dv_scr[...] += dv_blk

    def bwd_block(step, carry):
        j, t0 = ORDER[0], SLOTS[0]
        for k in range(1, len(ORDER)):
            past = (step + nb - k) // nb
            j = j + (ORDER[k] - ORDER[k - 1]) * past
            t0 = t0 + (SLOTS[k] - SLOTS[k - 1]) * past
        g = j // per
        odd = lax.rem(j, per)
        off = mul(odd * BLK, BLK)

        def body(i, cc):
            hook(t0 + (i - g))

            @pl.when((i == g) & (odd == 1))
            def _():
                high = pl.ds(mul(g * piece + BLK, BLK), BLK)
                bwd_core(j, high, kt_scr[g, :, BLK:], cut(BLK, BLK), True, dqt_scr.at[g, :, BLK:])

            @pl.when((i == g) & (odd == 0))
            def _():
                bwd_core(j, pl.ds(mul(g * piece, piece), piece), kt_scr[g, :, :BLK], cut(BLK, piece), True, dqt_scr.at[g])

            @pl.when(i > g)
            def _():
                bwd_core(j, pl.ds(mul(i * piece, piece), piece), kt_scr[g, :, pl.ds(off, BLK)], None, False, dqt_scr.at[i])

            return cc

        lax.fori_loop(g, 4, body, 0)
        rows = blk(j)
        dk = dk_scr[...] * scale
        dkb = dk[:, :dn].astype(BF)
        dvb = dv_scr[...].astype(BF)
        dkv_scr[rows, :dn] = dkb
        dkv_scr[rows, dn:] = dvb
        dcp[rows, :] = mm_nt(dkv_scr[rows, :], wkv_scr[...])
        drt = dk[:, dn:].T
        owner = jnp.where((g == 0) | (g == 3), 0, 1)
        lt0 = (g // 2) * (piece // LANES) + odd * (BLK // LANES)
        lts = 2 * piece // LANES
        for rt in range(dr // 8):
            b, r = divmod(rt * lts * 8, BLK)
            for lt in range(BLK // LANES):
                row = mul(t_all + owner * BLK + r + (lt0 + lt) * 8, 8)
                dcp[pl.ds(row, 8), b * LANES:(b + 1) * LANES] = drt[rt * 8:rt * 8 + 8, lt * LANES:(lt + 1) * LANES]
        return carry

    def d_weights(lo_j, hi_j):
        def body(j, cc):
            rows = blk(j)
            dw_scr[...] += mm_tn(c_scr[rows, :], dkv_scr[rows, :])
            return cc

        lax.fori_loop(lo_j, hi_j, body, 0)

    def x_o(w):
        g = own_piece(w)
        far_g = (1 - me) if w == 0 else 2 + me
        return pltpu.make_async_remote_copy(src_ref=o_scr.at[pl.ds(mul(far_g * piece, piece), piece), :],
                                            dst_ref=o_far.at[pl.ds(w * piece, piece), :],
                                            send_sem=out_snd.at[w], recv_sem=out_rcv.at[w],
                                            device_id=mate, device_id_type=MESH)

    def x_w():
        return pltpu.make_async_remote_copy(src_ref=dw_scr, dst_ref=dw_far, send_sem=out_snd.at[2], recv_sem=out_rcv.at[2],
                                            device_id=mate, device_id_type=MESH)

    def x_q(w):
        far_g = (1 - me) if w == 0 else 2 + me
        return pltpu.make_async_remote_copy(src_ref=dqt_scr.at[far_g], dst_ref=dqt_out.at[me, :, pl.ds(w * piece, piece)],
                                            send_sem=out_snd.at[4 + w], recv_sem=out_rcv.at[4 + w],
                                            device_id=mate, device_id_type=MESH)

    for w in range(2):
        x_o(w).start()
    for g in range(4):
        dqt_scr[g] = jnp.zeros(dqt_scr.shape[1:], F32)
    dw_scr[...] = jnp.zeros_like(dw_scr)
    lax.fori_loop(0, nb, bwd_block, 0)

    def tail(k):
        for core in range(2):
            items = [(n, k + d) for c, n, d in TAIL if c == core and (k + d > 0) and k + d < n_stage]
            items += [(n, 0) for c, n, d in TAIL if c == 1 - core and k + d == 0]
            if items:
                run_for(core, items)

    tail(0)
    for g in range(4):
        dqt_scr[g] = dqt_scr[g] * scale
    tail(1)
    d_weights(0, nb // 2)
    tail(2)
    d_weights(nb // 2, nb)
    x_w().start()
    for w in range(2):
        x_q(w).start()
    tail(3)
    for w in range(2):
        dqt_out[me, :, pl.ds(w * piece, piece)] = dqt_scr[own_piece(w)]
    tail(4)
    for w in range(2):
        x_o(w).wait_recv()
        mine = o_scr[pl.ds(mul(own_piece(w) * piece, piece), piece), :]
        o_out[pl.ds(w * piece, piece)] = pack(dkv_scr.at[pl.ds(0, piece), :], mine, o_far[pl.ds(w * piece, piece), :])
    tail(5)
    x_w().wait_recv()
    for o_, lo_ in ((dwk_out, 0), (dwv_out, dn)):
        o_[...] = pack(wide_scr, dw_scr[:, lo_:lo_ + dn], dw_far[:, lo_:lo_ + dn])
    for k in range(6, n_stage):
        tail(k)
    for rt in range(dr // 8):
        for lt in range(2 * piece // LANES):
            b, r = divmod((rt * (2 * piece // LANES) + lt) * 8, BLK)
            r += 2 * piece
            drt_out[rt * 8:rt * 8 + 8, lt * LANES:(lt + 1) * LANES] = sum_out[r:r + 8, b * LANES:(b + 1) * LANES]
    for w in range(2):
        x_q(w).wait()
        x_o(w).wait_send()
        for k in range(4):
            in_remote(w, own_piece(w), k).wait_send()

    x_w().wait_send()

    for wh, n in ((0, cols), (1, cols), (2, cols), (3, cols), (4, 1)):
        def drain(b, cc, wh=wh):
            un = Unit(wh, b, 0)
            un.swap().wait_send()
            return cc

        lax.fori_loop(0, n, drain, 0)


def run(c, rt, qt, do, wuk, wuv, side, vmem=51 * 2**20):
    half, rank = c.shape
    t = 2 * half
    dr = rt.shape[0]
    qk = qt.shape[1]
    dn = wuk.shape[2]
    dv = wuv.shape[2]
    nb = t // BLK
    piece = t // 4
    nu = 4 * (rank // WIDE) + 1
    sds = jax.ShapeDtypeStruct
    vm = pltpu.VMEM
    bufs = []
    size = BLK
    for _ in range(3):
        n = size // side
        h = n // 2 if n % 16 == 0 else n
        bufs += [vm((nu, 2, h, WIDE), F32)] if not bufs else []
        bufs += [vm((nu, 2 if size == BLK else 3, n, WIDE), F32)]
        size = n
    dma = pltpu.SemaphoreType.DMA
    any_spec = pl.BlockSpec(memory_space=pl.ANY)
    vm_spec = pl.BlockSpec(memory_space=pltpu.VMEM)
    return pl.pallas_call(
        functools.partial(kernel, side),
        in_specs=[any_spec] * 4 + [vm_spec] * 2,
        out_specs=[vm_spec] * 6,
        out_shape=[vm((half, 2, dv), BF), vm((2, qk, half), F32), vm((half + BLK, rank), F32), vm((dr, half), F32),
                   vm((rank, 2, dn), F32), vm((rank, 2, dv), F32)],
        scratch_shapes=[vm((t, rank), BF), vm((dr, t), BF), vm((qk, t), BF), vm((t, 2, dv), BF), vm((rank, dn + dv), BF),
                        vm((t, dv), BF), vm((t, qk), BF), vm((t, dv), BF), vm((4, qk, piece), BF), vm((4, dv, piece), BF),
                        vm((t, dv), BF), vm((1, t), F32), vm((1, t), F32),
                        vm((1, piece), F32), vm((1, piece), F32), vm((dv, piece), F32), vm((4, qk, piece), F32),
                        vm((BLK, qk), F32), vm((BLK, dv), F32), vm((t, dn + dv), BF), vm((rank, 2 * dn), F32),
                        vm((t + 2 * BLK, rank), F32), vm((rank, dn + dv), F32),
                        vm((half, dv), BF), vm((rank, dn + dv), F32), vm((nu, BLK, WIDE), F32)]
        + bufs + [dma((4, 2)), dma((4, 2)), dma((4, 2)), dma((nu, 4)), dma((nu, 21)), dma((6,)), dma((6,))],
        compiler_params=pltpu.CompilerParams(collective_id=0, has_side_effects=True, vmem_limit_bytes=vmem),
        name="mla_step",
    )(c, rt, qt, do, wuk, wuv)


def store_kernel(*refs):
    n = (len(refs) - 1) // 2
    sem = refs[-1]
    copies = []
    for k in range(n):
        src, dst = refs[k], refs[n + k]
        if src.shape != dst.shape:
            src = src.at[pl.ds(0, dst.shape[0]), :]
        copies.append(pltpu.make_async_copy(src, dst, sem.at[k]))
    for cpy in copies:
        cpy.start()
    for cpy in copies:
        cpy.wait()


def store_all(arrays, shapes):
    n = len(arrays)
    return pl.pallas_call(
        store_kernel,
        in_specs=[pl.BlockSpec(memory_space=pltpu.VMEM)] * n,
        out_specs=[pl.BlockSpec(memory_space=pl.ANY)] * n,
        out_shape=[pltpu.HBM(sh, a.dtype) for a, sh in zip(arrays, shapes)],
        scratch_shapes=[pltpu.SemaphoreType.DMA((n,))],
        compiler_params=pltpu.CompilerParams(vmem_limit_bytes=2**20),
        name="store_all",
    )(*arrays)


def solution(mesh):
    side = round(mesh.shape['tp'] ** (1 / 3))
    seq_spec = P(('dp', 'cp'), None)
    head_spec = P(('dp', 'cp'), 'tp', None)
    weight_spec = P(None, 'tp', None)
    grad_spec = P('dp', 'tp', None)

    def device_fn(c_latent, k_rope, q_heads, d_out, w_uk, w_uv):
        outs = run(c_latent, k_rope.T, jnp.transpose(q_heads, (1, 2, 0)), d_out, w_uk, w_uv, side)
        shapes = [c_latent.shape if k == 2 else x.shape for k, x in enumerate(outs)]
        o, dqt, dc, drt, dwk, dwv = store_all(outs, shapes)
        return o, jnp.transpose(dqt, (2, 0, 1)), dc, drt.T, dwk, dwv

    return jax.shard_map(device_fn, mesh=mesh,
                         in_specs=(seq_spec, seq_spec, head_spec, head_spec, weight_spec, weight_spec),
                         out_specs=(head_spec, head_spec, seq_spec, seq_spec, grad_spec, grad_spec),
                         check_vma=False)
```
